512 devices in a mesh: pole: 8 (over z_lo), grid: 64 (over x, z_hi, y, core).
Axes of the slice: x: 4, y: 4, z: 16 (z_hi: 2, z_lo: 8; z = z_hi * 8 + z_lo), core: 2. Of those that a mesh axis runs over, the one named last changes fastest.
Arguments:
- inverse_rows: bfloat16 [8, 2, 8192, 8192], P('pole', None, 'grid'), may hold values from -0.09375 to 0.09375
- factor: bfloat16 [8, 2, 2048, 2, 512], P('pole', None, 'grid'), may hold values from -0.8984375 to 0.8984375
- diag_inverse: float32 [8, 2, 512, 2, 512], P('pole', None, None, None, 'grid'), may hold values from -6 to 6
- pole_weights: float32 [8, 2], P('pole'), may hold values from -3 to 3
- structure: int32 [2, 4], replicated, may hold values from 0 to 15, as said below
- row_owner: int32 [16], replicated, may hold values from 0 to 15, each once
Outputs:
- column_sum: float32 [2, 8192, 2, 512], P(None, 'grid', None, 'pole')
- diagonal_sum: float32 [2, 512, 2, 512], P(None, 'pole', None, 'grid')
The draws below stay inside these ranges and needn't reach their ends.
Inputs may be any that keep to these rules, and one draw needn't show every extreme that they name: `structure`: row k lists 4 distinct ancestors of supernode k in ascending order. A permutation: ancestor a's block row is stored as block row row_owner[a].
All inputs are finite; a program needn't handle non-finite values.
Results may differ from the reference program's by a relative error of at most 0.0029.
Values may be sent and summed in bfloat16 or wider, within the bound.
A program may use at most 64 MiB of HBM per device.

```python
import jax
import jax.numpy as jnp
from jax import lax

BLOCK = 512
ANCESTORS = 16
LISTED = 4
SNODES = 2
POLES = 8
N_POLE = 8


def draw_structure(key, part):
    listed_rows = []
    for snode_id in range(SNODES):
        shuffled = jax.random.permutation(jax.random.fold_in(key, 71 + snode_id), ANCESTORS)
        listed_rows.append(jnp.sort(shuffled[:LISTED]))
    return jnp.stack(listed_rows).astype(jnp.int32)


def block_levels(own_key, dims, cuts, smallest, top_value):
    factor_of, own = 1.0, jax.random.fold_in(own_key, 6)
    for dim, parts in cuts:
        steps = jnp.exp(jax.random.uniform(jax.random.fold_in(own, dim), (parts,), jnp.float32, smallest / len(cuts), top_value / len(cuts)))
        factor_of = factor_of * jnp.repeat(steps, dims[dim] // parts).reshape([-1 if axis == dim else 1 for axis in range(len(dims))])
    return factor_of


def noise(rng, shape, width, bound, split=(), held_as=jnp.bfloat16):
    loudness = block_levels(rng, shape, split, -0.22, 0.18) if split else 1.0
    array = jax.random.normal(rng, shape, jnp.float32) * width * loudness
    return jnp.minimum(jnp.maximum(array, -bound), bound).astype(held_as)


def setup_inputs(seed: int = 0) -> dict:
    seeds = jax.random.split(jax.random.key(seed), 7)
    return {
        "inverse_rows": noise(seeds[0], (POLES, 2, ANCESTORS * BLOCK, ANCESTORS * BLOCK), (2 * LISTED * BLOCK) ** -0.5, 0.09375, ((0, 8), (2, 64))),
        "factor": noise(seeds[1], (POLES, SNODES, LISTED * BLOCK, 2, BLOCK), 0.15, 0.8984375, ((0, 8), (2, 64))),
        "diag_inverse": noise(seeds[2], (POLES, SNODES, BLOCK, 2, BLOCK), 1.0, 6.0, ((0, 8), (4, 64)), jnp.float32),
        "pole_weights": noise(seeds[3], (POLES, 2), 0.5, 3.0, ((0, 8),), jnp.float32),
        "structure": draw_structure(jax.random.fold_in(seeds[6], 71), 0),
        "row_owner": jax.random.permutation(seeds[5], ANCESTORS).astype(jnp.int32),
    }


def complex_scale(weight_pair, values):
    real_part = values[..., 0, :]
    imag_part = values[..., 1, :]
    return jnp.stack([weight_pair[0] * real_part - weight_pair[1] * imag_part, weight_pair[0] * imag_part + weight_pair[1] * real_part], axis=-2)


def reference(inverse_rows, factor, diag_inverse, pole_weights, structure, row_owner):
    within = jnp.arange(BLOCK, dtype=jnp.int32)
    span_rows = LISTED * BLOCK
    column_total = jnp.zeros((SNODES, ANCESTORS * BLOCK, 2, BLOCK), jnp.float32)
    diagonal_total = jnp.zeros((SNODES, BLOCK, 2, BLOCK), jnp.float32)
    for pole_id in range(N_POLE):
        columns = []
        diagonals = []
        for snode_id in range(SNODES):
            listed = structure[snode_id].astype(jnp.int32)
            slot_ids = row_owner[listed].astype(jnp.int32)
            row_index = (slot_ids[:, None] * BLOCK + within[None, :]).reshape(-1).astype(jnp.int32)
            col_index = (listed[:, None] * BLOCK + within[None, :]).reshape(-1).astype(jnp.int32)
            chosen = jnp.take(jnp.take(inverse_rows[pole_id], row_index, axis=1), col_index, axis=2)
            factor_flat = factor[pole_id, snode_id].reshape(span_rows, 2 * BLOCK)
            product = jnp.dot(chosen.reshape(2 * span_rows, span_rows), factor_flat, preferred_element_type=jnp.float32)
            real_part = product[span_rows:, BLOCK:] - product[:span_rows, :BLOCK]
            imag_part = -(product[:span_rows, BLOCK:] + product[span_rows:, :BLOCK])
            column = jnp.stack([real_part, imag_part], axis=1)
            rounded_column = column.astype(jnp.bfloat16)
            placed = jnp.zeros((ANCESTORS * BLOCK, 2, BLOCK), jnp.float32).at[row_index].set(rounded_column.astype(jnp.float32))
            rounded = rounded_column.reshape(span_rows, 2 * BLOCK)
            moment = lax.dot_general(factor_flat, rounded, (((0,), (0,)), ((), ())), preferred_element_type=jnp.float32)
            diag_real = moment[:BLOCK, :BLOCK] - moment[BLOCK:, BLOCK:]
            diag_imag = moment[:BLOCK, BLOCK:] + moment[BLOCK:, :BLOCK]
            diagonal = diag_inverse[pole_id, snode_id] - jnp.stack([diag_real, diag_imag], axis=1)
            columns.append(placed)
            diagonals.append(diagonal)
        column_total = column_total + complex_scale(pole_weights[pole_id], jnp.stack(columns))
        diagonal_total = diagonal_total + complex_scale(pole_weights[pole_id], jnp.stack(diagonals))
    return column_total, diagonal_total
```

```python
import jax
import jax.numpy as jnp
from jax import lax
from jax.experimental import pallas as pl
from jax.experimental.pallas import tpu as pltpu
from jax.sharding import PartitionSpec as P

BLOCK = 512
LISTED = 4
SNODES = 2
POLES = 8
PLANES = 2
SIDE = 4
IN_PLANE = 32
RING = 16
LANES = 128
ROWS = 128
SHARD = 32
MESH = pl.DeviceIdType.MESH
DOT = (((1,), (0,)), ((), ()))

ORDER = (
    (0, 0), (1, 0), (0, 2), (2, 0), (1, 2), (3, 0), (2, 2), (0, 1), (4, 0), (3, 2), (1, 1), (4, 2),
    (0, 3), (2, 1), (1, 3), (3, 1), (2, 3), (4, 1), "first", (3, 3), (4, 3), "second",
)
ROUNDS = ((0, 0), (0, 1), (1, 0), (1, 1))


def kernel(
    structure, row_owner, weights, factor, rows_hbm, diag,
    column_out, diag_out,
    fbuf, rows, esend, erecv, tsend, trecv, dsend, drecv, wrows,
    rows_sem, ag_sem, cross_sem, pair_sem, erecv_sem, trecv_sem, drecv_sem, wrecv_sem,
    ag_sent, cross_sent, esent, tsent, dsent, wsent,
):
    pole = lax.axis_index("pole")
    grid = lax.axis_index("grid")
    x, plane = grid // 16, (grid // 8) % 2
    y, core = (grid // 2) % 4, grid % 2
    seat = x * 8 + y * 2 + core
    height = plane * 8 + pole

    def at(x_to, plane_to, y_to, core_to):
        return x_to * 16 + plane_to * 8 + y_to * 2 + core_to

    def along(first, second, core_to=core, plane_to=plane):
        x_to = (x + core * first + (1 - core) * second) % SIDE
        y_to = (y + (1 - core) * first + core * second) % SIDE
        return at(x_to, plane_to, y_to, core_to)

    def seat_grid(seat_to):
        return at(seat_to // 8, plane, (seat_to // 2) % 4, seat_to % 2)

    def height_device(height_to):
        return (height_to % 8, at(x, height_to // 8, y, core))

    load_rows = pltpu.make_async_copy(rows_hbm, rows, rows_sem)
    load_rows.start()

    part = lax.broadcasted_iota(jnp.int32, (8, LANES), 0)
    wrows[pole] = jnp.where(part == 0, weights[0, 0], weights[0, 1])

    barrier = pltpu.get_barrier_semaphore()

    def greet_seat(step, carry):
        target = seat_grid((seat + step) % IN_PLANE)
        pl.semaphore_signal(barrier, inc=1, device_id=(pole, target), device_id_type=MESH)
        return carry

    def greet_height(step, carry):
        target = height_device((height + step) % RING)
        pl.semaphore_signal(barrier, inc=1, device_id=target, device_id_type=MESH)
        return carry

    lax.fori_loop(1, IN_PLANE, greet_seat, 0)
    lax.fori_loop(1, RING, greet_height, 0)
    for k in range(SNODES):
        fbuf[k, grid] = factor[k]
    pl.semaphore_wait(barrier, IN_PLANE - 1 + RING - 1)

    def copy(src, dst, sent, received, device):
        return pltpu.make_async_remote_copy(
            src_ref=src, dst_ref=dst, send_sem=sent, recv_sem=received,
            device_id=device, device_id_type=MESH,
        )

    def cross(k):
        return copy(
            factor.at[k], fbuf.at[k, grid], cross_sent.at[k], cross_sem.at[k],
            height_device((height + 8) % RING),
        )

    for k in range(SNODES):
        cross(k).start()

    def wait_for(ref, sem):
        pltpu.make_async_copy(ref, ref, sem).wait()

    def push(r, src, slot, offset, sem_index):
        k = ROUNDS[r][0]
        first, second = offset
        copy(
            src, slot, ag_sent.at[k], ag_sem.at[r, sem_index],
            (pole, along(first, second)),
        ).start()

    def stage(step, r):
        k, other = ROUNDS[r]
        source_plane = plane if other == 0 else 1 - plane

        def shard(first, second):
            return fbuf.at[k, along(first, second, plane_to=source_plane)]

        def half(ref, which):
            return ref.at[pl.ds(16 * which, 16)]

        own = factor.at[k] if other == 0 else shard(0, 0)

        def to_sibling(src, first, second):
            copy(
                src, shard(first, second), ag_sent.at[k], pair_sem.at[k],
                (pole, at(x, plane, y, 1 - core)),
            ).start()

        def start_second(src, first, index):
            slot = shard(first, 0)
            push(r, src, slot, (0, 1), 4 + 4 * index)
            push(r, src, slot, (0, -1), 5 + 4 * index)

        def turn_second(first, index):
            base = 4 + 4 * index
            low = shard(first, -1)
            wait_for(low, ag_sem.at[r, base])
            push(r, half(low, 0), half(low, 0), (0, 1), base + 2)
            to_sibling(low, first, -1)
            high = shard(first, 1)
            wait_for(high, ag_sem.at[r, base + 1])
            push(r, half(high, 1), half(high, 1), (0, -1), base + 3)
            to_sibling(high, first, 1)

        def end_second(first, index):
            base = 4 + 4 * index
            far = shard(first, 2)
            wait_for(half(far, 0), ag_sem.at[r, base + 2])
            wait_for(half(far, 1), ag_sem.at[r, base + 3])
            to_sibling(far, first, 2)

        if step == 0:
            if other == 1:
                cross(k).wait_recv()
            push(r, own, shard(0, 0), (1, 0), 0)
            push(r, own, shard(0, 0), (-1, 0), 1)
            start_second(own, 0, 0)
            to_sibling(own, 0, 0)
        if step == 1:
            low = shard(-1, 0)
            wait_for(low, ag_sem.at[r, 0])
            push(r, half(low, 0), half(low, 0), (1, 0), 2)
            start_second(low, -1, 1)
            to_sibling(low, -1, 0)
            high = shard(1, 0)
            wait_for(high, ag_sem.at[r, 1])
            push(r, half(high, 1), half(high, 1), (-1, 0), 3)
            start_second(high, 1, 2)
            to_sibling(high, 1, 0)
            turn_second(0, 0)
        if step == 2:
            far = shard(2, 0)
            wait_for(half(far, 0), ag_sem.at[r, 2])
            wait_for(half(far, 1), ag_sem.at[r, 3])
            start_second(far, 2, 3)
            to_sibling(far, 2, 0)
            turn_second(-1, 1)
            turn_second(1, 2)
            end_second(0, 0)
        if step == 3:
            turn_second(2, 3)
            end_second(-1, 1)
            end_second(1, 2)
        if step == 4:
            end_second(2, 3)

    lane = lax.broadcasted_iota(jnp.int32, (1, LANES), 1)
    sign = jnp.where(lane < 64, -1.0, 1.0).astype(jnp.float32)

    def turned(values):
        return sign * pltpu.roll(values, 64, 1)

    def weight_send(step):
        return copy(
            wrows.at[pole], wrows.at[pole], wsent, wrecv_sem,
            ((pole + step) % POLES, grid),
        )

    def columns(k):
        wait_for(fbuf.at[k, pl.ds(0, IN_PLANE)], pair_sem.at[k])
        active = 0
        for i in range(LISTED):
            active = active + jnp.where(owners[k][i] == grid // 4, 1, 0)
        active = active.astype(jnp.float32)
        for n in range(4):
            product = jnp.zeros((2 * ROWS, 2 * LANES), jnp.float32)
            for i in range(LISTED):
                start = structure[k, i] * BLOCK
                block = fbuf[k, pl.ds(16 * i, 16), :, pl.ds(256 * n, 256)].reshape(BLOCK, 256)
                product = product + lax.dot_general(
                    rows[:, pl.ds(start, BLOCK)], block, DOT, preferred_element_type=jnp.float32
                )
            flipped = []
            for u in range(2):
                lanes = slice(LANES * u, LANES * (u + 1))
                value = -(product[:ROWS, lanes] + turned(product[ROWS:, lanes]))
                rounded = (value * active).astype(jnp.bfloat16)
                esend[k, 2 * n + u] = rounded
                flipped.append(jnp.transpose(rounded.astype(jnp.float32)))
            for h in range(8):
                pieces = [
                    flipped[u][64 * part_id + 8 * h : 64 * part_id + 8 * h + 8]
                    for part_id in range(2)
                    for u in range(2)
                ]
                tsend[k, 8 * n + h] = jnp.concatenate(pieces, axis=0).astype(jnp.bfloat16)

        def send_column(step, carry):
            target = (pole + step) % POLES
            copy(
                esend.at[k, target], erecv.at[k, pole], esent.at[k], erecv_sem.at[k],
                (target, grid),
            ).start()
            return carry

        def send_tile(step, carry):
            target = (seat + step) % IN_PLANE
            copy(
                tsend.at[k, target], trecv.at[k, seat], tsent.at[k], trecv_sem.at[k],
                (pole, seat_grid(target)),
            ).start()
            return carry

        lax.fori_loop(1, IN_PLANE, send_tile, 0)
        lax.fori_loop(1, POLES, send_column, 0)
        erecv[k, pole] = esend[k, pole]
        trecv[k, seat] = tsend[k, seat]

    def moments(k):
        wait_for(trecv.at[k, pl.ds(0, IN_PLANE - 1)], trecv_sem.at[k])
        total = jnp.zeros((SHARD, 2 * BLOCK), jnp.float32)
        for i in range(LISTED):
            left = jnp.zeros((SHARD, BLOCK), jnp.bfloat16)
            for slot in range(8):
                place = (slot // 2) * 4 + plane * 2 + slot % 2
                here = jnp.where(owners[k][i] == place, 1.0, 0.0).astype(jnp.bfloat16)
                tiles = [trecv[k, 4 * slot + q] for q in range(4)]
                left = left + here * jnp.concatenate(tiles, axis=1)
            block = fbuf[k, pl.ds(16 * i, 16)].reshape(BLOCK, 2 * BLOCK)
            total = total + lax.dot_general(left, block, DOT, preferred_element_type=jnp.float32)
        weight_real, weight_imag = weights[0, 0], weights[0, 1]
        for j in range(POLES):
            lanes = slice(LANES * j, LANES * (j + 1))
            moment = total[:16, lanes] + turned(total[16:, lanes])
            for side in range(2):
                mine = jnp.where(plane == side, 1.0, 0.0).astype(jnp.float32)
                value = mine * diag[k, :, lanes] - moment[8 * side : 8 * side + 8]
                dsend[8 * side + j, k] = weight_real * value + weight_imag * turned(value)

    owners = []
    for k in range(SNODES):
        owners.append([])
        for i in range(LISTED):
            owner = 0
            for ancestor in range(16):
                owner = owner + jnp.where(structure[k, i] == ancestor, row_owner[ancestor], 0)
            owners[k].append(owner)

    for step in range(1, POLES):
        weight_send(step).start()

    for entry in ORDER:
        if entry == "first":
            load_rows.wait()
            columns(0)
        elif entry == "second":
            columns(1)
        else:
            stage(*entry)

    for k in range(SNODES):
        moments(k)

    def send_diag(step, carry):
        target = (height + step) % RING
        copy(
            dsend.at[target], drecv.at[height], dsent, drecv_sem, height_device(target)
        ).start()
        return carry

    lax.fori_loop(1, RING, send_diag, 0)
    drecv[height] = dsend[height]

    wait_for(wrows.at[pl.ds(0, POLES - 1)], wrecv_sem)
    for k in range(SNODES):
        wait_for(erecv.at[k, pl.ds(0, POLES - 1)], erecv_sem.at[k])
        straight = jnp.zeros((ROWS, LANES), jnp.float32)
        crossed = jnp.zeros((ROWS, LANES), jnp.float32)
        for p in range(POLES):
            value = erecv[k, p].astype(jnp.float32)
            straight = straight + wrows[p, 0:1, :] * value
            crossed = crossed + wrows[p, 1:2, :] * value
        column_out[k] = straight + turned(crossed)

    wait_for(drecv.at[pl.ds(0, RING - 1)], drecv_sem)
    summed = drecv[0]
    for source in range(1, RING):
        summed = summed + drecv[source]
    diag_out[...] = summed

    for k in range(SNODES):
        cross(k).wait_send()
        wait_for(fbuf.at[k, pl.ds(0, 62)], ag_sent.at[k])
        wait_for(esend.at[k, pl.ds(0, POLES - 1)], esent.at[k])
        wait_for(tsend.at[k, pl.ds(0, IN_PLANE - 1)], tsent.at[k])
    wait_for(dsend.at[pl.ds(0, RING - 1)], dsent)
    wait_for(wrows.at[pl.ds(0, POLES - 1)], wsent)


def body(inverse_rows, factor, diag_inverse, pole_weights, structure, row_owner):
    rows = inverse_rows.reshape(2 * ROWS, inverse_rows.shape[3])
    by_pole = factor.reshape(SNODES, SHARD, 2, POLES, 64).transpose(0, 1, 3, 2, 4)
    by_pole = by_pole.reshape(SNODES, SHARD, 2 * BLOCK)
    diag = diag_inverse.reshape(SNODES, POLES, 64, 2, 8).transpose(0, 4, 1, 3, 2)
    diag = diag.reshape(SNODES, 8, 2 * BLOCK)
    smem = pl.BlockSpec(memory_space=pltpu.SMEM)
    vmem = pl.BlockSpec(memory_space=pltpu.VMEM)
    dma = pltpu.SemaphoreType.DMA
    column, diagonal = pl.pallas_call(
        kernel,
        out_shape=(
            jax.ShapeDtypeStruct((SNODES, ROWS, LANES), jnp.float32),
            jax.ShapeDtypeStruct((SNODES, 8, LANES), jnp.float32),
        ),
        in_specs=[smem, smem, smem, vmem, pl.BlockSpec(memory_space=pl.ANY), vmem],
        out_specs=(vmem, vmem),
        scratch_shapes=[
            pltpu.VMEM((SNODES, 64, SHARD, 2 * BLOCK), jnp.bfloat16),
            pltpu.VMEM((2 * ROWS, 8192), jnp.bfloat16),
            pltpu.VMEM((SNODES, POLES, ROWS, LANES), jnp.bfloat16),
            pltpu.VMEM((SNODES, POLES, ROWS, LANES), jnp.bfloat16),
            pltpu.VMEM((SNODES, IN_PLANE, SHARD, LANES), jnp.bfloat16),
            pltpu.VMEM((SNODES, IN_PLANE, SHARD, LANES), jnp.bfloat16),
            pltpu.VMEM((RING, SNODES, 8, LANES), jnp.float32),
            pltpu.VMEM((RING, SNODES, 8, LANES), jnp.float32),
            pltpu.VMEM((POLES, 8, LANES), jnp.float32),
            dma,
            dma((4, 20)),
            dma((SNODES,)),
            dma((SNODES,)),
            dma((SNODES,)),
            dma((SNODES,)),
            dma,
            dma,
            dma((SNODES,)),
            dma((SNODES,)),
            dma((SNODES,)),
            dma((SNODES,)),
            dma,
            dma,
        ],
        compiler_params=pltpu.CompilerParams(
            collective_id=0, has_side_effects=True, vmem_limit_bytes=48 * 1024 * 1024
        ),
    )(structure, row_owner, pole_weights, by_pole, rows, diag)
    column_sum = column.reshape(SNODES, ROWS, 2, 64)
    diagonal_sum = diagonal.reshape(SNODES, 8, 2, 64).transpose(0, 3, 2, 1)
    return (column_sum, diagonal_sum)


def solution(mesh):
    in_specs = (
        P("pole", None, "grid", None),
        P("pole", None, "grid", None, None),
        P("pole", None, None, None, "grid"),
        P("pole", None),
        P(),
        P(),
    )
    out_specs = (P(None, "grid", None, "pole"), P(None, "pole", None, "grid"))
    return jax.shard_map(body, mesh=mesh, in_specs=in_specs, out_specs=out_specs, check_vma=False)
```

```python
import jax
import jax.numpy as jnp
from jax import lax
from jax.experimental import pallas as pl
from jax.experimental.pallas import tpu as pltpu
from jax.sharding import PartitionSpec as P

BLOCK = 512
LISTED = 4
SNODES = 2
POLES = 8
PLANES = 2
SIDE = 4
IN_PLANE = 32
RING = 16
LANES = 128
ROWS = 128
SHARD = 32
MESH = pl.DeviceIdType.MESH
DOT = (((1,), (0,)), ((), ()))

ORDER = (
    (0, 0), (0, 2), (1, 0), (1, 2), (2, 0), (2, 2), (3, 0), (0, 1), (3, 2), (4, 0), (1, 1), (4, 2),
    (0, 3), (2, 1), (1, 3), (3, 1), (2, 3), (4, 1), (3, 3), "first", (4, 3), "second", "moments",
)
ROUNDS = ((0, 0), (0, 1), (1, 0), (1, 1))


def kernel(
    structure_hbm, row_owner_hbm, weights_hbm, factor, rows_hbm, diag,
    column_out, diag_out,
    structure, row_owner, weights, small_sem, fbuf, rows, esend, erecv, tsend, trecv, dsend, drecv, wrows,
    rows_sem, ag_sem, cross_sem, pair_sem, erecv_sem, trecv_sem, drecv_sem, wrecv_sem,
    ag_sent, cross_sent, esent, tsent, dsent, wsent,
):
    pole = lax.axis_index("pole")
    grid = lax.axis_index("grid")
    x, plane = grid // 16, (grid // 8) % 2
    y, core = (grid // 2) % 4, grid % 2
    seat = x * 8 + y * 2 + core
    height = plane * 8 + pole

    def at(x_to, plane_to, y_to, core_to):
        return x_to * 16 + plane_to * 8 + y_to * 2 + core_to

    def along(first, second, core_to=core, plane_to=plane):
        x_to = (x + core * first + (1 - core) * second) % SIDE
        y_to = (y + (1 - core) * first + core * second) % SIDE
        return at(x_to, plane_to, y_to, core_to)

    def seat_grid(seat_to):
        return at(seat_to // 8, plane, (seat_to // 2) % 4, seat_to % 2)

    def height_device(height_to):
        return (height_to % 8, at(x, height_to // 8, y, core))

    load_rows = pltpu.make_async_copy(rows_hbm, rows, rows_sem)
    load_rows.start()
    small = [
        pltpu.make_async_copy(source, target, small_sem.at[i])
        for i, (source, target) in enumerate(
            ((structure_hbm, structure), (row_owner_hbm, row_owner), (weights_hbm, weights))
        )
    ]
    for load in small:
        load.start()

    barrier = pltpu.get_barrier_semaphore()

    def greet_seat(step, carry):
        target = seat_grid((seat + step) % IN_PLANE)
        pl.semaphore_signal(barrier, inc=1, device_id=(pole, target), device_id_type=MESH)
        return carry

    def greet_height(step, carry):
        target = height_device((height + step) % RING)
        pl.semaphore_signal(barrier, inc=1, device_id=target, device_id_type=MESH)
        return carry

    lax.fori_loop(1, IN_PLANE, greet_seat, 0)
    lax.fori_loop(1, RING, greet_height, 0)
    for k in range(SNODES):
        fbuf[k, grid] = factor[k]
    for load in small:
        load.wait()
    part = lax.broadcasted_iota(jnp.int32, (8, LANES), 0)
    wrows[pole] = jnp.where(part == 0, weights[0, 0], weights[0, 1])
    pl.semaphore_wait(barrier, IN_PLANE - 1 + RING - 1)

    def copy(src, dst, sent, received, device):
        return pltpu.make_async_remote_copy(
            src_ref=src, dst_ref=dst, send_sem=sent, recv_sem=received,
            device_id=device, device_id_type=MESH,
        )

    def cross(k):
        return copy(
            factor.at[k], fbuf.at[k, grid], cross_sent.at[k], cross_sem.at[k],
            height_device((height + 8) % RING),
        )

    for k in range(SNODES):
        cross(k).start()

    def wait_for(ref, sem):
        pltpu.make_async_copy(ref, ref, sem).wait()

    def push(r, src, slot, offset, sem_index):
        k = ROUNDS[r][0]
        first, second = offset
        copy(
            src, slot, ag_sent.at[k], ag_sem.at[r, sem_index],
            (pole, along(first, second)),
        ).start()

    def stage(step, r):
        k, other = ROUNDS[r]
        source_plane = plane if other == 0 else 1 - plane

        def shard(first, second):
            return fbuf.at[k, along(first, second, plane_to=source_plane)]

        def half(ref, which):
            return ref.at[pl.ds(16 * which, 16)]

        own = factor.at[k] if other == 0 else shard(0, 0)

        def to_sibling(src, first, second):
            copy(
                src, shard(first, second), ag_sent.at[k], pair_sem.at[k],
                (pole, at(x, plane, y, 1 - core)),
            ).start()

        def start_second(src, first, index):
            slot = shard(first, 0)
            push(r, src, slot, (0, 1), 4 + 4 * index)
            push(r, src, slot, (0, -1), 5 + 4 * index)

        def turn_second(first, index):
            base = 4 + 4 * index
            low = shard(first, -1)
            wait_for(low, ag_sem.at[r, base])
            push(r, half(low, 0), half(low, 0), (0, 1), base + 2)
            to_sibling(low, first, -1)
            high = shard(first, 1)
            wait_for(high, ag_sem.at[r, base + 1])
            push(r, half(high, 1), half(high, 1), (0, -1), base + 3)
            to_sibling(high, first, 1)

        def end_second(first, index):
            base = 4 + 4 * index
            far = shard(first, 2)
            wait_for(half(far, 0), ag_sem.at[r, base + 2])
            wait_for(half(far, 1), ag_sem.at[r, base + 3])
            to_sibling(far, first, 2)

        if step == 0:
            if other == 1:
                cross(k).wait_recv()
            push(r, own, shard(0, 0), (1, 0), 0)
            push(r, own, shard(0, 0), (-1, 0), 1)
            start_second(own, 0, 0)
            to_sibling(own, 0, 0)
        if step == 1:
            low = shard(-1, 0)
            wait_for(low, ag_sem.at[r, 0])
            push(r, half(low, 0), half(low, 0), (1, 0), 2)
            start_second(low, -1, 1)
            to_sibling(low, -1, 0)
            high = shard(1, 0)
            wait_for(high, ag_sem.at[r, 1])
            push(r, half(high, 1), half(high, 1), (-1, 0), 3)
            start_second(high, 1, 2)
            to_sibling(high, 1, 0)
            turn_second(0, 0)
        if step == 2:
            far = shard(2, 0)
            wait_for(half(far, 0), ag_sem.at[r, 2])
            wait_for(half(far, 1), ag_sem.at[r, 3])
            start_second(far, 2, 3)
            to_sibling(far, 2, 0)
            turn_second(-1, 1)
            turn_second(1, 2)
            end_second(0, 0)
        if step == 3:
            turn_second(2, 3)
            end_second(-1, 1)
            end_second(1, 2)
        if step == 4:
            end_second(2, 3)

    lane = lax.broadcasted_iota(jnp.int32, (1, LANES), 1)
    sign = jnp.where(lane < 64, -1.0, 1.0).astype(jnp.float32)

    def turned(values):
        return sign * pltpu.roll(values, 64, 1)

    def weight_send(step):
        return copy(
            wrows.at[pole], wrows.at[pole], wsent, wrecv_sem,
            ((pole + step) % POLES, grid),
        )

    def columns(k):
        wait_for(fbuf.at[k, pl.ds(0, IN_PLANE)], pair_sem.at[k])
        active = 0
        for i in range(LISTED):
            active = active + jnp.where(owners[k][i] == grid // 4, 1, 0)
        active = active.astype(jnp.float32)

        def chunk(step, carry):
            n = (x + 1 + step) % SIDE
            start = pl.multiple_of(2 * LANES * n, 2 * LANES)
            product = jnp.zeros((2 * ROWS, 2 * LANES), jnp.float32)
            for i in range(LISTED):
                block = fbuf[k, pl.ds(16 * i, 16), :, pl.ds(start, 2 * LANES)]
                product = product + lax.dot_general(
                    rows[:, pl.ds(structure[k, i] * BLOCK, BLOCK)],
                    block.reshape(BLOCK, 2 * LANES),
                    DOT,
                    preferred_element_type=jnp.float32,
                )
            flipped = []
            for u in range(2):
                lanes = slice(LANES * u, LANES * (u + 1))
                value = -(product[:ROWS, lanes] + turned(product[ROWS:, lanes]))
                rounded = (value * active).astype(jnp.bfloat16)
                esend[k, 2 * n + u] = rounded
                flipped.append(jnp.transpose(rounded.astype(jnp.float32)))
            for h in range(8):
                pieces = [
                    flipped[u][64 * part_id + 8 * h : 64 * part_id + 8 * h + 8]
                    for part_id in range(2)
                    for u in range(2)
                ]
                tsend[k, 8 * n + h] = jnp.concatenate(pieces, axis=0).astype(jnp.bfloat16)

            def send_tile(h, inner):
                target = 8 * n + (y * 2 + core + 1 + h) % 8

                @pl.when(target != seat)
                def _():
                    copy(
                        tsend.at[k, target], trecv.at[k, seat], tsent.at[k], trecv_sem.at[k],
                        (pole, seat_grid(target)),
                    ).start()

                return inner

            lax.fori_loop(0, 8, send_tile, 0)
            for u in range(2):
                target = 2 * n + u

                @pl.when(target != pole)
                def _(target=target):
                    copy(
                        esend.at[k, target], erecv.at[k, pole], esent.at[k], erecv_sem.at[k],
                        (target, grid),
                    ).start()

            return carry

        lax.fori_loop(0, SIDE, chunk, 0)
        erecv[k, pole] = esend[k, pole]
        trecv[k, seat] = tsend[k, seat]

    def moments(k):
        wait_for(trecv.at[k, pl.ds(0, IN_PLANE - 1)], trecv_sem.at[k])
        total = jnp.zeros((SHARD, 2 * BLOCK), jnp.float32)
        for i in range(LISTED):
            left = jnp.zeros((SHARD, BLOCK), jnp.bfloat16)
            for slot in range(8):
                place = (slot // 2) * 4 + plane * 2 + slot % 2
                here = jnp.where(owners[k][i] == place, 1.0, 0.0).astype(jnp.bfloat16)
                tiles = [trecv[k, 4 * slot + q] for q in range(4)]
                left = left + here * jnp.concatenate(tiles, axis=1)
            block = fbuf[k, pl.ds(16 * i, 16)].reshape(BLOCK, 2 * BLOCK)
            total = total + lax.dot_general(left, block, DOT, preferred_element_type=jnp.float32)
        weight_real, weight_imag = weights[0, 0], weights[0, 1]
        for j in range(POLES):
            lanes = slice(LANES * j, LANES * (j + 1))
            moment = total[:16, lanes] + turned(total[16:, lanes])
            at_128 = slice(LANES * (j // 2), LANES * (j // 2 + 1))
            diag_real, diag_imag = diag[k, 0, :, at_128], diag[k, 1, :, at_128]
            if j % 2 == 0:
                given = jnp.where(lane < 64, diag_real, pltpu.roll(diag_imag, 64, 1))
            else:
                given = jnp.where(lane < 64, pltpu.roll(diag_real, 64, 1), diag_imag)
            for side in range(2):
                mine = jnp.where(plane == side, 1.0, 0.0).astype(jnp.float32)
                value = mine * given - moment[8 * side : 8 * side + 8]
                dsend[k, 8 * side + j] = weight_real * value + weight_imag * turned(value)

        def send_diag(step, carry):
            target = (height + step) % RING
            copy(
                dsend.at[k, target], drecv.at[k, height], dsent.at[k], drecv_sem.at[k],
                height_device(target),
            ).start()
            return carry

        lax.fori_loop(1, RING, send_diag, 0)
        drecv[k, height] = dsend[k, height]

    def sum_columns(k):
        wait_for(erecv.at[k, pl.ds(0, POLES - 1)], erecv_sem.at[k])
        straight = jnp.zeros((ROWS, LANES), jnp.float32)
        crossed = jnp.zeros((ROWS, LANES), jnp.float32)
        for p in range(POLES):
            value = erecv[k, p].astype(jnp.float32)
            straight = straight + wrows[p, 0:1, :] * value
            crossed = crossed + wrows[p, 1:2, :] * value
        flat = jnp.transpose(straight + turned(crossed))
        column_out[k, 0] = flat[:64]
        column_out[k, 1] = flat[64:]

    owners = []
    for k in range(SNODES):
        owners.append([])
        for i in range(LISTED):
            owner = 0
            for ancestor in range(16):
                owner = owner + jnp.where(structure[k, i] == ancestor, row_owner[ancestor], 0)
            owners[k].append(owner)

    for step in range(1, POLES):
        weight_send(step).start()

    for entry in ORDER:
        if entry == "first":
            load_rows.wait()
            columns(0)
        elif entry == "second":
            columns(1)
        elif entry == "moments":
            moments(0)
        else:
            stage(*entry)

    moments(1)
    wait_for(wrows.at[pl.ds(0, POLES - 1)], wrecv_sem)
    sum_columns(0)
    sum_columns(1)
    for k in range(SNODES):
        wait_for(drecv.at[k, pl.ds(0, RING - 1)], drecv_sem.at[k])
        summed = drecv[k, 0]
        for source in range(1, RING):
            summed = summed + drecv[k, source]
        diag_out[k, 0] = summed[:, :64]
        diag_out[k, 1] = pltpu.roll(summed, 64, 1)[:, :64]

    for k in range(SNODES):
        cross(k).wait_send()
        wait_for(fbuf.at[k, pl.ds(0, 62)], ag_sent.at[k])
        wait_for(esend.at[k, pl.ds(0, POLES - 1)], esent.at[k])
        wait_for(tsend.at[k, pl.ds(0, IN_PLANE - 1)], tsent.at[k])
        wait_for(dsend.at[k, pl.ds(0, RING - 1)], dsent.at[k])
    wait_for(wrows.at[pl.ds(0, POLES - 1)], wsent)


def body(inverse_rows, factor, diag_inverse, pole_weights, structure, row_owner):
    rows = inverse_rows.reshape(2 * ROWS, inverse_rows.shape[3])
    by_pole = factor.reshape(SNODES, SHARD, 2, POLES, 64).transpose(0, 1, 3, 2, 4)
    by_pole = by_pole.reshape(SNODES, SHARD, 2 * BLOCK)
    diag = diag_inverse[0].transpose(0, 2, 3, 1)
    hbm = pl.BlockSpec(memory_space=pltpu.HBM)
    vmem = pl.BlockSpec(memory_space=pltpu.VMEM)
    dma = pltpu.SemaphoreType.DMA
    column, diagonal = pl.pallas_call(
        kernel,
        out_shape=(
            jax.ShapeDtypeStruct((SNODES, 2, 64, ROWS), jnp.float32),
            jax.ShapeDtypeStruct((SNODES, 2, 8, 64), jnp.float32),
        ),
        in_specs=[hbm, hbm, hbm, vmem, hbm, vmem],
        out_specs=(vmem, vmem),
        scratch_shapes=[
            pltpu.SMEM((SNODES, LISTED), jnp.int32),
            pltpu.SMEM((16,), jnp.int32),
            pltpu.SMEM((1, 2), jnp.float32),
            dma((3,)),
            pltpu.VMEM((SNODES, 64, SHARD, 2 * BLOCK), jnp.bfloat16),
            pltpu.VMEM((2 * ROWS, 8192), jnp.bfloat16),
            pltpu.VMEM((SNODES, POLES, ROWS, LANES), jnp.bfloat16),
            pltpu.VMEM((SNODES, POLES, ROWS, LANES), jnp.bfloat16),
            pltpu.VMEM((SNODES, IN_PLANE, SHARD, LANES), jnp.bfloat16),
            pltpu.VMEM((SNODES, IN_PLANE, SHARD, LANES), jnp.bfloat16),
            pltpu.VMEM((SNODES, RING, 8, LANES), jnp.float32),
            pltpu.VMEM((SNODES, RING, 8, LANES), jnp.float32),
            pltpu.VMEM((POLES, 8, LANES), jnp.float32),
            dma,
            dma((4, 20)),
            dma((SNODES,)),
            dma((SNODES,)),
            dma((SNODES,)),
            dma((SNODES,)),
            dma((SNODES,)),
            dma,
            dma((SNODES,)),
            dma((SNODES,)),
            dma((SNODES,)),
            dma((SNODES,)),
            dma((SNODES,)),
            dma,
        ],
        compiler_params=pltpu.CompilerParams(
            collective_id=0, has_side_effects=True, vmem_limit_bytes=60 * 1024 * 1024
        ),
    )(structure, row_owner, pole_weights, by_pole, rows, diag)
    column_sum = column.transpose(0, 3, 1, 2)
    diagonal_sum = diagonal.transpose(0, 3, 1, 2)
    return (column_sum, diagonal_sum)


def solution(mesh):
    in_specs = (
        P("pole", None, "grid", None),
        P("pole", None, "grid", None, None),
        P("pole", None, None, None, "grid"),
        P("pole", None),
        P(),
        P(),
    )
    out_specs = (P(None, "grid", None, "pole"), P(None, "pole", None, "grid"))
    return jax.shard_map(body, mesh=mesh, in_specs=in_specs, out_specs=out_specs, check_vma=False)
```

```python
import jax
import jax.numpy as jnp
from jax import lax
from jax.experimental import pallas as pl
from jax.experimental.pallas import tpu as pltpu
from jax.sharding import PartitionSpec as P

BLOCK = 512
LISTED = 4
SNODES = 2
POLES = 8
HALF = 4
PLANES = 2
SIDE = 4
IN_PLANE = 32
RING = 16
LANES = 128
ROWS = 128
SHARD = 32
MESH = pl.DeviceIdType.MESH
DOT = (((1,), (0,)), ((), ()))

ORDER = (
    (0, 0), (0, 2), (1, 0), (1, 2), (2, 0), (2, 2), (3, 0), (0, 1), (3, 2), (4, 0), (1, 1), (4, 2),
    (0, 3), (2, 1), (1, 3), (3, 1), (2, 3), (4, 1), (3, 3), "first", (4, 3), "second", "moments",
)
ROUNDS = ((0, 0), (0, 1), (1, 0), (1, 1))


def kernel(
    structure_hbm, row_owner_hbm, weights_hbm, factor, rows_hbm, diag,
    column_out, diag_out,
    structure, row_owner, weights, small_sem, fbuf, rows, esend, erecv, psend, precv, tsend, trecv, dsend, drecv, wrows,
    rows_sem, ag_sem, cross_sem, pair_sem, erecv_sem, precv_sem, trecv_sem, drecv_sem, wrecv_sem,
    ag_sent, cross_sent, esent, psent, tsent, dsent, wsent,
):
    pole = lax.axis_index("pole")
    grid = lax.axis_index("grid")
    x, plane = grid // 16, (grid // 8) % 2
    y, core = (grid // 2) % 4, grid % 2
    seat = x * 8 + y * 2 + core
    height = plane * 8 + pole
    quad, member = pole // HALF, pole % HALF

    def at(x_to, plane_to, y_to, core_to):
        return x_to * 16 + plane_to * 8 + y_to * 2 + core_to

    def along(first, second, core_to=core, plane_to=plane):
        x_to = (x + core * first + (1 - core) * second) % SIDE
        y_to = (y + (1 - core) * first + core * second) % SIDE
        return at(x_to, plane_to, y_to, core_to)

    def seat_grid(seat_to):
        return at(seat_to // 8, plane, (seat_to // 2) % 4, seat_to % 2)

    def height_device(height_to):
        return (height_to % 8, at(x, height_to // 8, y, core))

    load_rows = pltpu.make_async_copy(rows_hbm, rows, rows_sem)
    load_rows.start()
    small = [
        pltpu.make_async_copy(source, target, small_sem.at[i])
        for i, (source, target) in enumerate(
            ((structure_hbm, structure), (row_owner_hbm, row_owner), (weights_hbm, weights))
        )
    ]
    for load in small:
        load.start()

    barrier = pltpu.get_barrier_semaphore()

    def greet_seat(step, carry):
        target = seat_grid((seat + step) % IN_PLANE)
        pl.semaphore_signal(barrier, inc=1, device_id=(pole, target), device_id_type=MESH)
        return carry

    def greet_height(step, carry):
        target = height_device((height + step) % RING)
        pl.semaphore_signal(barrier, inc=1, device_id=target, device_id_type=MESH)
        return carry

    lax.fori_loop(1, IN_PLANE, greet_seat, 0)
    lax.fori_loop(1, RING, greet_height, 0)
    for k in range(SNODES):
        fbuf[k, grid] = factor[k]
    for load in small:
        load.wait()
    part = lax.broadcasted_iota(jnp.int32, (8, LANES), 0)
    wrows[pole] = jnp.where(part == 0, weights[0, 0], weights[0, 1])
    pl.semaphore_wait(barrier, IN_PLANE - 1 + RING - 1)

    def copy(src, dst, sent, received, device):
        return pltpu.make_async_remote_copy(
            src_ref=src, dst_ref=dst, send_sem=sent, recv_sem=received,
            device_id=device, device_id_type=MESH,
        )

    def cross(k):
        return copy(
            factor.at[k], fbuf.at[k, grid], cross_sent.at[k], cross_sem.at[k],
            height_device((height + 8) % RING),
        )

    for k in range(SNODES):
        cross(k).start()

    def wait_for(ref, sem):
        pltpu.make_async_copy(ref, ref, sem).wait()

    def push(r, src, slot, offset, sem_index):
        k = ROUNDS[r][0]
        first, second = offset
        copy(
            src, slot, ag_sent.at[k], ag_sem.at[r, sem_index],
            (pole, along(first, second)),
        ).start()

    def stage(step, r):
        k, other = ROUNDS[r]
        source_plane = plane if other == 0 else 1 - plane

        def shard(first, second):
            return fbuf.at[k, along(first, second, plane_to=source_plane)]

        def half(ref, which):
            return ref.at[pl.ds(16 * which, 16)]

        own = factor.at[k] if other == 0 else shard(0, 0)

        def to_sibling(src, first, second):
            copy(
                src, shard(first, second), ag_sent.at[k], pair_sem.at[k],
                (pole, at(x, plane, y, 1 - core)),
            ).start()

        def start_second(src, first, index):
            slot = shard(first, 0)
            push(r, src, slot, (0, 1), 4 + 4 * index)
            push(r, src, slot, (0, -1), 5 + 4 * index)

        def turn_second(first, index):
            base = 4 + 4 * index
            low = shard(first, -1)
            wait_for(low, ag_sem.at[r, base])
            push(r, half(low, 0), half(low, 0), (0, 1), base + 2)
            to_sibling(low, first, -1)
            high = shard(first, 1)
            wait_for(high, ag_sem.at[r, base + 1])
            push(r, half(high, 1), half(high, 1), (0, -1), base + 3)
            to_sibling(high, first, 1)

        def end_second(first, index):
            base = 4 + 4 * index
            far = shard(first, 2)
            wait_for(half(far, 0), ag_sem.at[r, base + 2])
            wait_for(half(far, 1), ag_sem.at[r, base + 3])
            to_sibling(far, first, 2)

        if step == 0:
            if other == 1:
                cross(k).wait_recv()
            push(r, own, shard(0, 0), (1, 0), 0)
            push(r, own, shard(0, 0), (-1, 0), 1)
            start_second(own, 0, 0)
            to_sibling(own, 0, 0)
        if step == 1:
            low = shard(-1, 0)
            wait_for(low, ag_sem.at[r, 0])
            push(r, half(low, 0), half(low, 0), (1, 0), 2)
            start_second(low, -1, 1)
            to_sibling(low, -1, 0)
            high = shard(1, 0)
            wait_for(high, ag_sem.at[r, 1])
            push(r, half(high, 1), half(high, 1), (-1, 0), 3)
            start_second(high, 1, 2)
            to_sibling(high, 1, 0)
            turn_second(0, 0)
        if step == 2:
            far = shard(2, 0)
            wait_for(half(far, 0), ag_sem.at[r, 2])
            wait_for(half(far, 1), ag_sem.at[r, 3])
            start_second(far, 2, 3)
            to_sibling(far, 2, 0)
            turn_second(-1, 1)
            turn_second(1, 2)
            end_second(0, 0)
        if step == 3:
            turn_second(2, 3)
            end_second(-1, 1)
            end_second(1, 2)
        if step == 4:
            end_second(2, 3)

    lane = lax.broadcasted_iota(jnp.int32, (1, LANES), 1)
    sign = jnp.where(lane < 64, -1.0, 1.0).astype(jnp.float32)

    def turned(values):
        return sign * pltpu.roll(values, 64, 1)

    def weight_send(step):
        return copy(
            wrows.at[pole], wrows.at[pole], wsent, wrecv_sem,
            (quad * HALF + (member + step) % HALF, grid),
        )

    def columns(k):
        wait_for(fbuf.at[k, pl.ds(0, IN_PLANE)], pair_sem.at[k])
        active = 0
        for i in range(LISTED):
            active = active + jnp.where(owners[k][i] == grid // 4, 1, 0)
        active = active.astype(jnp.float32)

        def chunk(step, carry):
            n = (x + 1 + step) % SIDE
            start = pl.multiple_of(2 * LANES * n, 2 * LANES)
            product = jnp.zeros((2 * ROWS, 2 * LANES), jnp.float32)
            for i in range(LISTED):
                block = fbuf[k, pl.ds(16 * i, 16), :, pl.ds(start, 2 * LANES)]
                product = product + lax.dot_general(
                    rows[:, pl.ds(structure[k, i] * BLOCK, BLOCK)],
                    block.reshape(BLOCK, 2 * LANES),
                    DOT,
                    preferred_element_type=jnp.float32,
                )
            flipped = []
            for u in range(2):
                lanes = slice(LANES * u, LANES * (u + 1))
                value = -(product[:ROWS, lanes] + turned(product[ROWS:, lanes]))
                rounded = (value * active).astype(jnp.bfloat16)
                esend[k, 2 * n + u] = rounded
                flipped.append(jnp.transpose(rounded.astype(jnp.float32)))
            for h in range(8):
                pieces = [
                    flipped[u][64 * part_id + 8 * h : 64 * part_id + 8 * h + 8]
                    for part_id in range(2)
                    for u in range(2)
                ]
                tsend[k, 8 * n + h] = jnp.concatenate(pieces, axis=0).astype(jnp.bfloat16)

            def send_tile(h, inner):
                target = 8 * n + (y * 2 + core + 1 + h) % 8

                @pl.when(target != seat)
                def _():
                    copy(
                        tsend.at[k, target], trecv.at[k, seat], tsent.at[k], trecv_sem.at[k],
                        (pole, seat_grid(target)),
                    ).start()

                return inner

            lax.fori_loop(0, 8, send_tile, 0)
            for u in range(2):
                chunk_id = 2 * n + u
                owner = chunk_id % HALF
                slot = (chunk_id // HALF) * HALF + member

                @pl.when(owner != member)
                def _(chunk_id=chunk_id, owner=owner, slot=slot):
                    copy(
                        esend.at[k, chunk_id], erecv.at[k, slot], esent.at[k], erecv_sem.at[k],
                        (quad * HALF + owner, grid),
                    ).start()

            return carry

        lax.fori_loop(0, SIDE, chunk, 0)
        for part in range(2):
            erecv[k, part * HALF + member] = esend[k, part * HALF + member]
        trecv[k, seat] = tsend[k, seat]

    def moments(k):
        wait_for(trecv.at[k, pl.ds(0, IN_PLANE - 1)], trecv_sem.at[k])
        total = jnp.zeros((SHARD, 2 * BLOCK), jnp.float32)
        for i in range(LISTED):
            left = jnp.zeros((SHARD, BLOCK), jnp.bfloat16)
            for slot in range(8):
                place = (slot // 2) * 4 + plane * 2 + slot % 2
                here = jnp.where(owners[k][i] == place, 1.0, 0.0).astype(jnp.bfloat16)
                tiles = [trecv[k, 4 * slot + q] for q in range(4)]
                left = left + here * jnp.concatenate(tiles, axis=1)
            block = fbuf[k, pl.ds(16 * i, 16)].reshape(BLOCK, 2 * BLOCK)
            total = total + lax.dot_general(left, block, DOT, preferred_element_type=jnp.float32)
        weight_real, weight_imag = weights[0, 0], weights[0, 1]
        for j in range(POLES):
            lanes = slice(LANES * j, LANES * (j + 1))
            moment = total[:16, lanes] + turned(total[16:, lanes])
            at_128 = slice(LANES * (j // 2), LANES * (j // 2 + 1))
            diag_real, diag_imag = diag[k, 0, :, at_128], diag[k, 1, :, at_128]
            if j % 2 == 0:
                given = jnp.where(lane < 64, diag_real, pltpu.roll(diag_imag, 64, 1))
            else:
                given = jnp.where(lane < 64, pltpu.roll(diag_real, 64, 1), diag_imag)
            for side in range(2):
                mine = jnp.where(plane == side, 1.0, 0.0).astype(jnp.float32)
                value = mine * given - moment[8 * side : 8 * side + 8]
                dsend[k, 8 * side + j] = weight_real * value + weight_imag * turned(value)

        def send_diag(step, carry):
            target = (height + step) % RING
            copy(
                dsend.at[k, target], drecv.at[k, height], dsent.at[k], drecv_sem.at[k],
                height_device(target),
            ).start()
            return carry

        lax.fori_loop(1, RING, send_diag, 0)
        drecv[k, height] = dsend[k, height]

    def partner_send(k):
        return copy(
            psend.at[k], precv.at[k], psent.at[k], precv_sem.at[k],
            ((pole + HALF) % POLES, grid),
        )

    def half_sum(k, part):
        straight = jnp.zeros((ROWS, LANES), jnp.float32)
        crossed = jnp.zeros((ROWS, LANES), jnp.float32)
        for r in range(HALF):
            value = erecv[k, part * HALF + r].astype(jnp.float32)
            straight = straight + wrows[quad * HALF + r, 0:1, :] * value
            crossed = crossed + wrows[quad * HALF + r, 1:2, :] * value
        return straight + turned(crossed)

    def send_half(k):
        wait_for(erecv.at[k, pl.ds(0, 2 * HALF - 2)], erecv_sem.at[k])
        psend[k] = half_sum(k, 1 - quad).astype(jnp.bfloat16)
        partner_send(k).start()

    def sum_columns(k):
        own = half_sum(k, quad)
        partner_send(k).wait_recv()
        flat = jnp.transpose(own + precv[k].astype(jnp.float32))
        column_out[k, 0] = flat[:64]
        column_out[k, 1] = flat[64:]

    owners = []
    for k in range(SNODES):
        owners.append([])
        for i in range(LISTED):
            owner = 0
            for ancestor in range(16):
                owner = owner + jnp.where(structure[k, i] == ancestor, row_owner[ancestor], 0)
            owners[k].append(owner)

    for step in range(1, HALF):
        weight_send(step).start()

    for entry in ORDER:
        if entry == "first":
            load_rows.wait()
            columns(0)
        elif entry == "second":
            columns(1)
        elif entry == "moments":
            moments(0)
        else:
            stage(*entry)

    wait_for(wrows.at[pl.ds(0, HALF - 1)], wrecv_sem)
    send_half(0)
    moments(1)
    send_half(1)
    sum_columns(0)
    sum_columns(1)
    for k in range(SNODES):
        wait_for(drecv.at[k, pl.ds(0, RING - 1)], drecv_sem.at[k])
        summed = drecv[k, 0]
        for source in range(1, RING):
            summed = summed + drecv[k, source]
        diag_out[k, 0] = summed[:, :64]
        diag_out[k, 1] = pltpu.roll(summed, 64, 1)[:, :64]

    for k in range(SNODES):
        cross(k).wait_send()
        wait_for(fbuf.at[k, pl.ds(0, 62)], ag_sent.at[k])
        wait_for(esend.at[k, pl.ds(0, 2 * HALF - 2)], esent.at[k])
        partner_send(k).wait_send()
        wait_for(tsend.at[k, pl.ds(0, IN_PLANE - 1)], tsent.at[k])
        wait_for(dsend.at[k, pl.ds(0, RING - 1)], dsent.at[k])
    wait_for(wrows.at[pl.ds(0, HALF - 1)], wsent)


def body(inverse_rows, factor, diag_inverse, pole_weights, structure, row_owner):
    rows = inverse_rows.reshape(2 * ROWS, inverse_rows.shape[3])
    by_pole = factor.reshape(SNODES, SHARD, 2, POLES, 64).transpose(0, 1, 3, 2, 4)
    by_pole = by_pole.reshape(SNODES, SHARD, 2 * BLOCK)
    diag = diag_inverse[0].transpose(0, 2, 3, 1)
    hbm = pl.BlockSpec(memory_space=pltpu.HBM)
    vmem = pl.BlockSpec(memory_space=pltpu.VMEM)
    dma = pltpu.SemaphoreType.DMA
    column, diagonal = pl.pallas_call(
        kernel,
        out_shape=(
            jax.ShapeDtypeStruct((SNODES, 2, 64, ROWS), jnp.float32),
            jax.ShapeDtypeStruct((SNODES, 2, 8, 64), jnp.float32),
        ),
        in_specs=[hbm, hbm, hbm, vmem, hbm, vmem],
        out_specs=(vmem, vmem),
        scratch_shapes=[
            pltpu.SMEM((SNODES, LISTED), jnp.int32),
            pltpu.SMEM((16,), jnp.int32),
            pltpu.SMEM((1, 2), jnp.float32),
            dma((3,)),
            pltpu.VMEM((SNODES, 64, SHARD, 2 * BLOCK), jnp.bfloat16),
            pltpu.VMEM((2 * ROWS, 8192), jnp.bfloat16),
            pltpu.VMEM((SNODES, POLES, ROWS, LANES), jnp.bfloat16),
            pltpu.VMEM((SNODES, POLES, ROWS, LANES), jnp.bfloat16),
            pltpu.VMEM((SNODES, ROWS, LANES), jnp.bfloat16),
            pltpu.VMEM((SNODES, ROWS, LANES), jnp.bfloat16),
            pltpu.VMEM((SNODES, IN_PLANE, SHARD, LANES), jnp.bfloat16),
            pltpu.VMEM((SNODES, IN_PLANE, SHARD, LANES), jnp.bfloat16),
            pltpu.VMEM((SNODES, RING, 8, LANES), jnp.float32),
            pltpu.VMEM((SNODES, RING, 8, LANES), jnp.float32),
            pltpu.VMEM((POLES, 8, LANES), jnp.float32),
            dma,
            dma((4, 20)),
            dma((SNODES,)),
            dma((SNODES,)),
            dma((SNODES,)),
            dma((SNODES,)),
            dma((SNODES,)),
            dma((SNODES,)),
            dma,
            dma((SNODES,)),
            dma((SNODES,)),
            dma((SNODES,)),
            dma((SNODES,)),
            dma((SNODES,)),
            dma((SNODES,)),
            dma,
        ],
        compiler_params=pltpu.CompilerParams(
            collective_id=0, has_side_effects=True, vmem_limit_bytes=60 * 1024 * 1024
        ),
    )(structure, row_owner, pole_weights, by_pole, rows, diag)
    column_sum = column.transpose(0, 3, 1, 2)
    diagonal_sum = diagonal.transpose(0, 3, 1, 2)
    return (column_sum, diagonal_sum)


def solution(mesh):
    in_specs = (
        P("pole", None, "grid", None),
        P("pole", None, "grid", None, None),
        P("pole", None, None, None, "grid"),
        P("pole", None),
        P(),
        P(),
    )
    out_specs = (P(None, "grid", None, "pole"), P(None, "pole", None, "grid"))
    return jax.shard_map(body, mesh=mesh, in_specs=in_specs, out_specs=out_specs, check_vma=False)
```

```python
import jax
import jax.numpy as jnp
from jax import lax
from jax.experimental import pallas as pl
from jax.experimental.pallas import tpu as pltpu
from jax.sharding import PartitionSpec as P

BLOCK = 512
LISTED = 4
SNODES = 2
POLES = 8
HALF = 4
PLANES = 2
SIDE = 4
IN_PLANE = 32
RING = 16
LANES = 128
ROWS = 128
SHARD = 32
MESH = pl.DeviceIdType.MESH
DOT = (((1,), (0,)), ((), ()))

ORDER = (
    (0, 0), (0, 2), (1, 0), (1, 2), (2, 0), (2, 2), (3, 0), (0, 1), (3, 2), (4, 0), (1, 1), (4, 2),
    (0, 3), (2, 1), (1, 3), (3, 1), (2, 3), (4, 1), (3, 3), "first", (4, 3), "second", "moments",
)
ROUNDS = ((0, 0), (0, 1), (1, 0), (1, 1))


def kernel(
    structure_hbm, row_owner_hbm, weights_hbm, factor, rows_hbm, diag,
    column_out, diag_out,
    structure, row_owner, weights, small_sem, fbuf, rows, esend, erecv, psend, precv, tsend, trecv, dsend, drecv, wrows,
    rows_sem, ag_sem, cross_sem, pair_sem, erecv_sem, precv_sem, trecv_sem, drecv_sem, wrecv_sem,
    ag_sent, cross_sent, esent, psent, tsent, dsent, wsent,
):
    pole = lax.axis_index("pole")
    grid = lax.axis_index("grid")
    x, plane = grid // 16, (grid // 8) % 2
    y, core = (grid // 2) % 4, grid % 2
    seat = x * 8 + y * 2 + core
    height = plane * 8 + pole
    quad, member = pole // HALF, pole % HALF

    def at(x_to, plane_to, y_to, core_to):
        return x_to * 16 + plane_to * 8 + y_to * 2 + core_to

    def along(first, second, core_to=core, plane_to=plane):
        x_to = (x + core * first + (1 - core) * second) % SIDE
        y_to = (y + (1 - core) * first + core * second) % SIDE
        return at(x_to, plane_to, y_to, core_to)

    def seat_grid(seat_to):
        return at(seat_to // 8, plane, (seat_to // 2) % 4, seat_to % 2)

    def height_device(height_to):
        return (height_to % 8, at(x, height_to // 8, y, core))

    load_rows = pltpu.make_async_copy(rows_hbm, rows, rows_sem)
    load_rows.start()
    small = [
        pltpu.make_async_copy(source, target, small_sem.at[i])
        for i, (source, target) in enumerate(
            ((structure_hbm, structure), (row_owner_hbm, row_owner), (weights_hbm, weights))
        )
    ]
    for load in small:
        load.start()

    barrier = pltpu.get_barrier_semaphore()

    def greet_seat(step, carry):
        target = seat_grid((seat + step) % IN_PLANE)
        pl.semaphore_signal(barrier, inc=1, device_id=(pole, target), device_id_type=MESH)
        return carry

    def greet_height(step, carry):
        target = height_device((height + step) % RING)
        pl.semaphore_signal(barrier, inc=1, device_id=target, device_id_type=MESH)
        return carry

    lax.fori_loop(1, IN_PLANE, greet_seat, 0)
    lax.fori_loop(1, RING, greet_height, 0)
    for k in range(SNODES):
        fbuf[k, grid] = factor[k]
    for load in small:
        load.wait()
    part = lax.broadcasted_iota(jnp.int32, (8, LANES), 0)
    wrows[pole] = jnp.where(part == 0, weights[0, 0], weights[0, 1])
    pl.semaphore_wait(barrier, IN_PLANE - 1 + RING - 1)

    def copy(src, dst, sent, received, device):
        return pltpu.make_async_remote_copy(
            src_ref=src, dst_ref=dst, send_sem=sent, recv_sem=received,
            device_id=device, device_id_type=MESH,
        )

    def cross(k):
        return copy(
            factor.at[k], fbuf.at[k, grid], cross_sent.at[k], cross_sem.at[k],
            height_device((height + 8) % RING),
        )

    for k in range(SNODES):
        cross(k).start()

    def wait_for(ref, sem):
        pltpu.make_async_copy(ref, ref, sem).wait()

    def push(r, src, slot, offset, sem_index):
        k = ROUNDS[r][0]
        first, second = offset
        copy(
            src, slot, ag_sent.at[k], ag_sem.at[r, sem_index],
            (pole, along(first, second)),
        ).start()

    def stage(step, r):
        k, other = ROUNDS[r]
        source_plane = plane if other == 0 else 1 - plane

        def shard(first, second):
            return fbuf.at[k, along(first, second, plane_to=source_plane)]

        def half(ref, which):
            return ref.at[pl.ds(16 * which, 16)]

        own = factor.at[k] if other == 0 else shard(0, 0)

        def to_sibling(src, first, second):
            copy(
                src, shard(first, second), ag_sent.at[k], pair_sem.at[k],
                (pole, at(x, plane, y, 1 - core)),
            ).start()

        def start_second(src, first, index):
            slot = shard(first, 0)
            push(r, src, slot, (0, 1), 4 + 4 * index)
            push(r, src, slot, (0, -1), 5 + 4 * index)

        def turn_second(first, index):
            base = 4 + 4 * index
            low = shard(first, -1)
            wait_for(low, ag_sem.at[r, base])
            push(r, half(low, 0), half(low, 0), (0, 1), base + 2)
            to_sibling(low, first, -1)
            high = shard(first, 1)
            wait_for(high, ag_sem.at[r, base + 1])
            push(r, half(high, 1), half(high, 1), (0, -1), base + 3)
            to_sibling(high, first, 1)

        def end_second(first, index):
            base = 4 + 4 * index
            far = shard(first, 2)
            wait_for(half(far, 0), ag_sem.at[r, base + 2])
            wait_for(half(far, 1), ag_sem.at[r, base + 3])
            to_sibling(far, first, 2)

        if step == 0:
            if other == 1:
                cross(k).wait_recv()
            push(r, own, shard(0, 0), (1, 0), 0)
            push(r, own, shard(0, 0), (-1, 0), 1)
            start_second(own, 0, 0)
            to_sibling(own, 0, 0)
        if step == 1:
            low = shard(-1, 0)
            wait_for(low, ag_sem.at[r, 0])
            push(r, half(low, 0), half(low, 0), (1, 0), 2)
            start_second(low, -1, 1)
            to_sibling(low, -1, 0)
            high = shard(1, 0)
            wait_for(high, ag_sem.at[r, 1])
            push(r, half(high, 1), half(high, 1), (-1, 0), 3)
            start_second(high, 1, 2)
            to_sibling(high, 1, 0)
            turn_second(0, 0)
        if step == 2:
            far = shard(2, 0)
            wait_for(half(far, 0), ag_sem.at[r, 2])
            wait_for(half(far, 1), ag_sem.at[r, 3])
            start_second(far, 2, 3)
            to_sibling(far, 2, 0)
            turn_second(-1, 1)
            turn_second(1, 2)
            end_second(0, 0)
        if step == 3:
            turn_second(2, 3)
            end_second(-1, 1)
            end_second(1, 2)
        if step == 4:
            end_second(2, 3)

    lane = lax.broadcasted_iota(jnp.int32, (1, LANES), 1)
    sign = jnp.where(lane < 64, -1.0, 1.0).astype(jnp.float32)

    def turned(values):
        return sign * pltpu.roll(values, 64, 1)

    def weight_send(step):
        return copy(
            wrows.at[pole], wrows.at[pole], wsent, wrecv_sem,
            (quad * HALF + (member + step) % HALF, grid),
        )

    def columns(k):
        wait_for(fbuf.at[k, pl.ds(0, IN_PLANE)], pair_sem.at[k])
        active = 0
        for i in range(LISTED):
            active = active + jnp.where(owners[k][i] == grid // 4, 1, 0)
        active = active.astype(jnp.float32)

        def chunk(step, carry):
            n = (x + 1 + step) % SIDE
            start = pl.multiple_of(2 * LANES * n, 2 * LANES)
            product = jnp.zeros((2 * ROWS, 2 * LANES), jnp.float32)
            for i in range(LISTED):
                block = fbuf[k, pl.ds(16 * i, 16), :, pl.ds(start, 2 * LANES)]
                product = product + lax.dot_general(
                    rows[:, pl.ds(structure[k, i] * BLOCK, BLOCK)],
                    block.reshape(BLOCK, 2 * LANES),
                    DOT,
                    preferred_element_type=jnp.float32,
                )
            flipped = []
            for u in range(2):
                lanes = slice(LANES * u, LANES * (u + 1))
                value = -(product[:ROWS, lanes] + turned(product[ROWS:, lanes]))
                rounded = (value * active).astype(jnp.bfloat16)
                esend[k, 2 * n + u] = rounded
                flipped.append(jnp.transpose(rounded.astype(jnp.float32)))
            for h in range(8):
                pieces = [
                    flipped[u][64 * part_id + 8 * h : 64 * part_id + 8 * h + 8]
                    for part_id in range(2)
                    for u in range(2)
                ]
                tsend[k, 8 * n + h] = jnp.concatenate(pieces, axis=0).astype(jnp.bfloat16)

            def send_tile(h, inner):
                target = 8 * n + (y * 2 + core + 1 + h) % 8

                @pl.when(target != seat)
                def _():
                    copy(
                        tsend.at[k, target], trecv.at[k, seat], tsent.at[k], trecv_sem.at[k],
                        (pole, seat_grid(target)),
                    ).start()

                return inner

            lax.fori_loop(0, 8, send_tile, 0)
            for u in range(2):
                chunk_id = 2 * n + u
                owner = chunk_id % HALF
                slot = (chunk_id // HALF) * HALF + member

                @pl.when(owner != member)
                def _(chunk_id=chunk_id, owner=owner, slot=slot):
                    copy(
                        esend.at[k, chunk_id], erecv.at[k, slot], esent.at[k], erecv_sem.at[k],
                        (quad * HALF + owner, grid),
                    ).start()

            return carry

        lax.fori_loop(0, SIDE, chunk, 0)
        for part in range(2):
            erecv[k, part * HALF + member] = esend[k, part * HALF + member]
        trecv[k, seat] = tsend[k, seat]

    def moments(k):
        wait_for(trecv.at[k, pl.ds(0, IN_PLANE - 1)], trecv_sem.at[k])
        total = jnp.zeros((SHARD, 2 * BLOCK), jnp.float32)
        for i in range(LISTED):
            left = jnp.zeros((SHARD, BLOCK), jnp.bfloat16)
            for slot in range(8):
                place = (slot // 2) * 4 + plane * 2 + slot % 2
                here = jnp.where(owners[k][i] == place, 1.0, 0.0).astype(jnp.bfloat16)
                tiles = [trecv[k, 4 * slot + q] for q in range(4)]
                left = left + here * jnp.concatenate(tiles, axis=1)
            block = fbuf[k, pl.ds(16 * i, 16)].reshape(BLOCK, 2 * BLOCK)
            total = total + lax.dot_general(left, block, DOT, preferred_element_type=jnp.float32)
        weight_real, weight_imag = weights[0, 0], weights[0, 1]
        for j in range(POLES):
            lanes = slice(LANES * j, LANES * (j + 1))
            moment = total[:16, lanes] + turned(total[16:, lanes])
            at_128 = slice(LANES * (j // 2), LANES * (j // 2 + 1))
            diag_real, diag_imag = diag[k, 0, :, at_128], diag[k, 1, :, at_128]
            if j % 2 == 0:
                given = jnp.where(lane < 64, diag_real, pltpu.roll(diag_imag, 64, 1))
            else:
                given = jnp.where(lane < 64, pltpu.roll(diag_real, 64, 1), diag_imag)
            for side in range(2):
                mine = jnp.where(plane == side, 1.0, 0.0).astype(jnp.float32)
                value = mine * given - moment[8 * side : 8 * side + 8]
                weighted = weight_real * value + weight_imag * turned(value)
                dsend[k, 8 * side + j] = weighted.astype(jnp.bfloat16)

        def send_diag(step, carry):
            target = (height + step) % RING
            copy(
                dsend.at[k, target], drecv.at[k, height], dsent.at[k], drecv_sem.at[k],
                height_device(target),
            ).start()
            return carry

        lax.fori_loop(1, RING, send_diag, 0)
        drecv[k, height] = dsend[k, height]

    def partner_send(k):
        return copy(
            psend.at[k], precv.at[k], psent.at[k], precv_sem.at[k],
            ((pole + HALF) % POLES, grid),
        )

    def half_sum(k, part):
        straight = jnp.zeros((ROWS, LANES), jnp.float32)
        crossed = jnp.zeros((ROWS, LANES), jnp.float32)
        for r in range(HALF):
            value = erecv[k, part * HALF + r].astype(jnp.float32)
            straight = straight + wrows[quad * HALF + r, 0:1, :] * value
            crossed = crossed + wrows[quad * HALF + r, 1:2, :] * value
        return straight + turned(crossed)

    def send_half(k):
        wait_for(erecv.at[k, pl.ds(0, 2 * HALF - 2)], erecv_sem.at[k])
        psend[k] = half_sum(k, 1 - quad).astype(jnp.bfloat16)
        partner_send(k).start()

    def sum_columns(k):
        own = half_sum(k, quad)
        partner_send(k).wait_recv()
        flat = jnp.transpose(own + precv[k].astype(jnp.float32))
        column_out[k, 0] = flat[:64]
        column_out[k, 1] = flat[64:]

    owners = []
    for k in range(SNODES):
        owners.append([])
        for i in range(LISTED):
            owner = 0
            for ancestor in range(16):
                owner = owner + jnp.where(structure[k, i] == ancestor, row_owner[ancestor], 0)
            owners[k].append(owner)

    for step in range(1, HALF):
        weight_send(step).start()

    for entry in ORDER:
        if entry == "first":
            load_rows.wait()
            columns(0)
        elif entry == "second":
            columns(1)
        elif entry == "moments":
            moments(0)
        else:
            stage(*entry)

    wait_for(wrows.at[pl.ds(0, HALF - 1)], wrecv_sem)
    send_half(0)
    moments(1)
    send_half(1)
    sum_columns(0)
    sum_columns(1)
    for k in range(SNODES):
        wait_for(drecv.at[k, pl.ds(0, RING - 1)], drecv_sem.at[k])
        summed = drecv[k, 0].astype(jnp.float32)
        for source in range(1, RING):
            summed = summed + drecv[k, source].astype(jnp.float32)
        diag_out[k, 0] = summed[:, :64]
        diag_out[k, 1] = pltpu.roll(summed, 64, 1)[:, :64]

    for k in range(SNODES):
        cross(k).wait_send()
        wait_for(fbuf.at[k, pl.ds(0, 62)], ag_sent.at[k])
        wait_for(esend.at[k, pl.ds(0, 2 * HALF - 2)], esent.at[k])
        partner_send(k).wait_send()
        wait_for(tsend.at[k, pl.ds(0, IN_PLANE - 1)], tsent.at[k])
        wait_for(dsend.at[k, pl.ds(0, RING - 1)], dsent.at[k])
    wait_for(wrows.at[pl.ds(0, HALF - 1)], wsent)


def body(inverse_rows, factor, diag_inverse, pole_weights, structure, row_owner):
    rows = inverse_rows.reshape(2 * ROWS, inverse_rows.shape[3])
    by_pole = factor.reshape(SNODES, SHARD, 2, POLES, 64).transpose(0, 1, 3, 2, 4)
    by_pole = by_pole.reshape(SNODES, SHARD, 2 * BLOCK)
    diag = diag_inverse[0].transpose(0, 2, 3, 1)
    hbm = pl.BlockSpec(memory_space=pltpu.HBM)
    vmem = pl.BlockSpec(memory_space=pltpu.VMEM)
    dma = pltpu.SemaphoreType.DMA
    column, diagonal = pl.pallas_call(
        kernel,
        out_shape=(
            pltpu.VMEM((SNODES, 2, 64, ROWS), jnp.float32),
            pltpu.VMEM((SNODES, 2, 8, 64), jnp.float32),
        ),
        in_specs=[hbm, hbm, hbm, vmem, hbm, vmem],
        out_specs=(vmem, vmem),
        scratch_shapes=[
            pltpu.SMEM((SNODES, LISTED), jnp.int32),
            pltpu.SMEM((16,), jnp.int32),
            pltpu.SMEM((1, 2), jnp.float32),
            dma((3,)),
            pltpu.VMEM((SNODES, 64, SHARD, 2 * BLOCK), jnp.bfloat16),
            pltpu.VMEM((2 * ROWS, 8192), jnp.bfloat16),
            pltpu.VMEM((SNODES, POLES, ROWS, LANES), jnp.bfloat16),
            pltpu.VMEM((SNODES, POLES, ROWS, LANES), jnp.bfloat16),
            pltpu.VMEM((SNODES, ROWS, LANES), jnp.bfloat16),
            pltpu.VMEM((SNODES, ROWS, LANES), jnp.bfloat16),
            pltpu.VMEM((SNODES, IN_PLANE, SHARD, LANES), jnp.bfloat16),
            pltpu.VMEM((SNODES, IN_PLANE, SHARD, LANES), jnp.bfloat16),
            pltpu.VMEM((SNODES, RING, 8, LANES), jnp.bfloat16),
            pltpu.VMEM((SNODES, RING, 8, LANES), jnp.bfloat16),
            pltpu.VMEM((POLES, 8, LANES), jnp.float32),
            dma,
            dma((4, 20)),
            dma((SNODES,)),
            dma((SNODES,)),
            dma((SNODES,)),
            dma((SNODES,)),
            dma((SNODES,)),
            dma((SNODES,)),
            dma,
            dma((SNODES,)),
            dma((SNODES,)),
            dma((SNODES,)),
            dma((SNODES,)),
            dma((SNODES,)),
            dma((SNODES,)),
            dma,
        ],
        compiler_params=pltpu.CompilerParams(
            collective_id=0, has_side_effects=True, vmem_limit_bytes=60 * 1024 * 1024
        ),
    )(structure, row_owner, pole_weights, by_pole, rows, diag)
    column_sum = column.transpose(0, 3, 1, 2)
    diagonal_sum = diagonal.transpose(0, 3, 1, 2)
    return (column_sum, diagonal_sum)


def solution(mesh):
    in_specs = (
        P("pole", None, "grid", None),
        P("pole", None, "grid", None, None),
        P("pole", None, None, None, "grid"),
        P("pole", None),
        P(),
        P(),
    )
    out_specs = (P(None, "grid", None, "pole"), P(None, "pole", None, "grid"))
    return jax.shard_map(body, mesh=mesh, in_specs=in_specs, out_specs=out_specs, check_vma=False)
```

```python
import jax
import jax.numpy as jnp
from jax import lax
from jax.experimental import pallas as pl
from jax.experimental.pallas import tpu as pltpu
from jax.sharding import PartitionSpec as P

BLOCK = 512
LISTED = 4
SNODES = 2
POLES = 8
HALF = 4
PLANES = 2
SIDE = 4
IN_PLANE = 32
RING = 16
LANES = 128
ROWS = 128
SHARD = 32
MESH = pl.DeviceIdType.MESH
DOT = (((1,), (0,)), ((), ()))

ORDER = (
    (0, 0), (0, 2), (1, 0), (1, 2), (2, 0), (2, 2), (3, 0), (0, 1), (3, 2), (4, 0), (1, 1), (4, 2),
    (0, 3), (2, 1), (1, 3), (3, 1), (2, 3), (4, 1), (3, 3), "first", (4, 3), "second", "moments",
)
ROUNDS = ((0, 0), (0, 1), (1, 0), (1, 1))


def kernel(
    structure_hbm, row_owner_hbm, weights_hbm, factor, rows_hbm, diag,
    column_out, diag_out,
    structure, row_owner, weights, small_sem, fbuf, rows, esend, erecv, psend, precv, tsend, trecv, dsend, drecv, wrows,
    rows_sem, ag_sem, cross_sem, pair_sem, erecv_sem, precv_sem, trecv_sem, drecv_sem, wrecv_sem,
    ag_sent, cross_sent, esent, psent, tsent, dsent, wsent,
):
    pole = lax.axis_index("pole")
    grid = lax.axis_index("grid")
    x, plane = grid // 16, (grid // 8) % 2
    y, core = (grid // 2) % 4, grid % 2
    seat = x * 8 + y * 2 + core
    height = plane * 8 + pole
    quad, member = pole // HALF, pole % HALF

    def at(x_to, plane_to, y_to, core_to):
        return x_to * 16 + plane_to * 8 + y_to * 2 + core_to

    def along(first, second, core_to=core, plane_to=plane):
        x_to = (x + core * first + (1 - core) * second) % SIDE
        y_to = (y + (1 - core) * first + core * second) % SIDE
        return at(x_to, plane_to, y_to, core_to)

    def seat_grid(seat_to):
        return at(seat_to // 8, plane, (seat_to // 2) % 4, seat_to % 2)

    def height_device(height_to):
        return (height_to % 8, at(x, height_to // 8, y, core))

    load_rows = pltpu.make_async_copy(rows_hbm, rows, rows_sem)
    load_rows.start()
    small = [
        pltpu.make_async_copy(source, target, small_sem.at[i])
        for i, (source, target) in enumerate(
            ((structure_hbm, structure), (row_owner_hbm, row_owner), (weights_hbm, weights))
        )
    ]
    for load in small:
        load.start()

    barrier = pltpu.get_barrier_semaphore()

    beside = [along(1, 0), along(-1, 0), along(0, 1), along(0, -1), at(x, plane, y, 1 - core)]

    def greet_height(step, carry):
        target = height_device((height + step) % RING)
        pl.semaphore_signal(barrier, inc=1, device_id=target, device_id_type=MESH)
        return carry

    for target in beside:
        pl.semaphore_signal(barrier, inc=1, device_id=(pole, target), device_id_type=MESH)
    lax.fori_loop(1, RING, greet_height, 0)
    for k in range(SNODES):
        fbuf[k, grid] = factor[k]
    for load in small:
        load.wait()
    part = lax.broadcasted_iota(jnp.int32, (8, LANES), 0)
    wrows[pole] = jnp.where(part == 0, weights[0, 0], weights[0, 1])
    pl.semaphore_wait(barrier, len(beside) + RING - 1)

    def copy(src, dst, sent, received, device):
        return pltpu.make_async_remote_copy(
            src_ref=src, dst_ref=dst, send_sem=sent, recv_sem=received,
            device_id=device, device_id_type=MESH,
        )

    def cross(k):
        return copy(
            factor.at[k], fbuf.at[k, grid], cross_sent.at[k], cross_sem.at[k],
            height_device((height + 8) % RING),
        )

    for k in range(SNODES):
        cross(k).start()

    def wait_for(ref, sem):
        pltpu.make_async_copy(ref, ref, sem).wait()

    def push(r, src, slot, offset, sem_index):
        k = ROUNDS[r][0]
        first, second = offset
        copy(
            src, slot, ag_sent.at[k], ag_sem.at[r, sem_index],
            (pole, along(first, second)),
        ).start()

    def stage(step, r):
        k, other = ROUNDS[r]
        source_plane = plane if other == 0 else 1 - plane

        def shard(first, second):
            return fbuf.at[k, along(first, second, plane_to=source_plane)]

        def half(ref, which):
            return ref.at[pl.ds(16 * which, 16)]

        own = factor.at[k] if other == 0 else shard(0, 0)

        def to_sibling(src, first, second):
            copy(
                src, shard(first, second), ag_sent.at[k], pair_sem.at[k],
                (pole, at(x, plane, y, 1 - core)),
            ).start()

        def start_second(src, first, index):
            slot = shard(first, 0)
            push(r, src, slot, (0, 1), 4 + 4 * index)
            push(r, src, slot, (0, -1), 5 + 4 * index)

        def turn_second(first, index):
            base = 4 + 4 * index
            low = shard(first, -1)
            wait_for(low, ag_sem.at[r, base])
            push(r, half(low, 0), half(low, 0), (0, 1), base + 2)
            to_sibling(low, first, -1)
            high = shard(first, 1)
            wait_for(high, ag_sem.at[r, base + 1])
            push(r, half(high, 1), half(high, 1), (0, -1), base + 3)
            to_sibling(high, first, 1)

        def end_second(first, index):
            base = 4 + 4 * index
            far = shard(first, 2)
            wait_for(half(far, 0), ag_sem.at[r, base + 2])
            wait_for(half(far, 1), ag_sem.at[r, base + 3])
            to_sibling(far, first, 2)

        if step == 0:
            if other == 1:
                cross(k).wait_recv()
            push(r, own, shard(0, 0), (1, 0), 0)
            push(r, own, shard(0, 0), (-1, 0), 1)
            start_second(own, 0, 0)
            to_sibling(own, 0, 0)
        if step == 1:
            low = shard(-1, 0)
            wait_for(low, ag_sem.at[r, 0])
            push(r, half(low, 0), half(low, 0), (1, 0), 2)
            start_second(low, -1, 1)
            to_sibling(low, -1, 0)
            high = shard(1, 0)
            wait_for(high, ag_sem.at[r, 1])
            push(r, half(high, 1), half(high, 1), (-1, 0), 3)
            start_second(high, 1, 2)
            to_sibling(high, 1, 0)
            turn_second(0, 0)
        if step == 2:
            far = shard(2, 0)
            wait_for(half(far, 0), ag_sem.at[r, 2])
            wait_for(half(far, 1), ag_sem.at[r, 3])
            start_second(far, 2, 3)
            to_sibling(far, 2, 0)
            turn_second(-1, 1)
            turn_second(1, 2)
            end_second(0, 0)
        if step == 3:
            turn_second(2, 3)
            end_second(-1, 1)
            end_second(1, 2)
        if step == 4:
            end_second(2, 3)

    lane = lax.broadcasted_iota(jnp.int32, (1, LANES), 1)
    sign = jnp.where(lane < 64, -1.0, 1.0).astype(jnp.float32)

    def turned(values):
        return sign * pltpu.roll(values, 64, 1)

    def weight_send(step):
        return copy(
            wrows.at[pole], wrows.at[pole], wsent, wrecv_sem,
            (quad * HALF + (member + step) % HALF, grid),
        )

    def columns(k):
        wait_for(fbuf.at[k, pl.ds(0, IN_PLANE)], pair_sem.at[k])
        active = 0
        for i in range(LISTED):
            active = active + jnp.where(owners[k][i] == grid // 4, 1, 0)
        active = active.astype(jnp.float32)

        def chunk(step, carry):
            n = (x + 1 + step) % SIDE
            start = pl.multiple_of(2 * LANES * n, 2 * LANES)
            product = jnp.zeros((2 * ROWS, 2 * LANES), jnp.float32)
            for i in range(LISTED):
                block = fbuf[k, pl.ds(16 * i, 16), :, pl.ds(start, 2 * LANES)]
                product = product + lax.dot_general(
                    rows[:, pl.ds(structure[k, i] * BLOCK, BLOCK)],
                    block.reshape(BLOCK, 2 * LANES),
                    DOT,
                    preferred_element_type=jnp.float32,
                )
            flipped = []
            for u in range(2):
                lanes = slice(LANES * u, LANES * (u + 1))
                value = -(product[:ROWS, lanes] + turned(product[ROWS:, lanes]))
                rounded = (value * active).astype(jnp.bfloat16)
                esend[k, 2 * n + u] = rounded
                flipped.append(jnp.transpose(rounded.astype(jnp.float32)))
            for h in range(8):
                pieces = [
                    flipped[u][64 * part_id + 8 * h : 64 * part_id + 8 * h + 8]
                    for part_id in range(2)
                    for u in range(2)
                ]
                tsend[k, 8 * n + h] = jnp.concatenate(pieces, axis=0).astype(jnp.bfloat16)

            def send_tile(h, inner):
                target = 8 * n + (y * 2 + core + 1 + h) % 8

                @pl.when(target != seat)
                def _():
                    copy(
                        tsend.at[k, target], trecv.at[k, seat], tsent.at[k], trecv_sem.at[k],
                        (pole, seat_grid(target)),
                    ).start()

                return inner

            lax.fori_loop(0, 8, send_tile, 0)
            for u in range(2):
                chunk_id = 2 * n + u
                owner = chunk_id % HALF
                slot = (chunk_id // HALF) * HALF + member

                @pl.when(owner != member)
                def _(chunk_id=chunk_id, owner=owner, slot=slot):
                    copy(
                        esend.at[k, chunk_id], erecv.at[k, slot], esent.at[k], erecv_sem.at[k],
                        (quad * HALF + owner, grid),
                    ).start()

            return carry

        lax.fori_loop(0, SIDE, chunk, 0)
        for part in range(2):
            erecv[k, part * HALF + member] = esend[k, part * HALF + member]
        trecv[k, seat] = tsend[k, seat]

    def moments(k):
        wait_for(trecv.at[k, pl.ds(0, IN_PLANE - 1)], trecv_sem.at[k])
        total = jnp.zeros((SHARD, 2 * BLOCK), jnp.float32)
        for i in range(LISTED):
            left = jnp.zeros((SHARD, BLOCK), jnp.bfloat16)
            for slot in range(8):
                place = (slot // 2) * 4 + plane * 2 + slot % 2
                here = jnp.where(owners[k][i] == place, 1.0, 0.0).astype(jnp.bfloat16)
                tiles = [trecv[k, 4 * slot + q] for q in range(4)]
                left = left + here * jnp.concatenate(tiles, axis=1)
            block = fbuf[k, pl.ds(16 * i, 16)].reshape(BLOCK, 2 * BLOCK)
            total = total + lax.dot_general(left, block, DOT, preferred_element_type=jnp.float32)
        weight_real, weight_imag = weights[0, 0], weights[0, 1]
        for j in range(POLES):
            lanes = slice(LANES * j, LANES * (j + 1))
            moment = total[:16, lanes] + turned(total[16:, lanes])
            at_128 = slice(LANES * (j // 2), LANES * (j // 2 + 1))
            diag_real, diag_imag = diag[k, 0, :, at_128], diag[k, 1, :, at_128]
            if j % 2 == 0:
                given = jnp.where(lane < 64, diag_real, pltpu.roll(diag_imag, 64, 1))
            else:
                given = jnp.where(lane < 64, pltpu.roll(diag_real, 64, 1), diag_imag)
            for side in range(2):
                mine = jnp.where(plane == side, 1.0, 0.0).astype(jnp.float32)
                value = mine * given - moment[8 * side : 8 * side + 8]
                weighted = weight_real * value + weight_imag * turned(value)
                dsend[k, 8 * side + j] = weighted.astype(jnp.bfloat16)

        def send_diag(step, carry):
            target = (height + step) % RING
            copy(
                dsend.at[k, target], drecv.at[k, height], dsent.at[k], drecv_sem.at[k],
                height_device(target),
            ).start()
            return carry

        lax.fori_loop(1, RING, send_diag, 0)
        drecv[k, height] = dsend[k, height]

    def partner_send(k):
        return copy(
            psend.at[k], precv.at[k], psent.at[k], precv_sem.at[k],
            ((pole + HALF) % POLES, grid),
        )

    def half_sum(k, part):
        straight = jnp.zeros((ROWS, LANES), jnp.float32)
        crossed = jnp.zeros((ROWS, LANES), jnp.float32)
        for r in range(HALF):
            value = erecv[k, part * HALF + r].astype(jnp.float32)
            straight = straight + wrows[quad * HALF + r, 0:1, :] * value
            crossed = crossed + wrows[quad * HALF + r, 1:2, :] * value
        return straight + turned(crossed)

    def send_half(k):
        wait_for(erecv.at[k, pl.ds(0, 2 * HALF - 2)], erecv_sem.at[k])
        psend[k] = half_sum(k, 1 - quad).astype(jnp.bfloat16)
        partner_send(k).start()

    def sum_columns(k):
        own = half_sum(k, quad)
        partner_send(k).wait_recv()
        flat = jnp.transpose(own + precv[k].astype(jnp.float32))
        column_out[k, 0] = flat[:64]
        column_out[k, 1] = flat[64:]

    owners = []
    for k in range(SNODES):
        owners.append([])
        for i in range(LISTED):
            owner = 0
            for ancestor in range(16):
                owner = owner + jnp.where(structure[k, i] == ancestor, row_owner[ancestor], 0)
            owners[k].append(owner)

    for step in range(1, HALF):
        weight_send(step).start()

    for entry in ORDER:
        if entry == "first":
            load_rows.wait()
            columns(0)
        elif entry == "second":
            columns(1)
        elif entry == "moments":
            moments(0)
        else:
            stage(*entry)

    wait_for(wrows.at[pl.ds(0, HALF - 1)], wrecv_sem)
    send_half(0)
    moments(1)
    send_half(1)
    sum_columns(0)
    sum_columns(1)
    for k in range(SNODES):
        wait_for(drecv.at[k, pl.ds(0, RING - 1)], drecv_sem.at[k])
        summed = drecv[k, 0].astype(jnp.float32)
        for source in range(1, RING):
            summed = summed + drecv[k, source].astype(jnp.float32)
        diag_out[k, 0] = summed[:, :64]
        diag_out[k, 1] = pltpu.roll(summed, 64, 1)[:, :64]

    for k in range(SNODES):
        cross(k).wait_send()
        wait_for(fbuf.at[k, pl.ds(0, 62)], ag_sent.at[k])
        wait_for(esend.at[k, pl.ds(0, 2 * HALF - 2)], esent.at[k])
        partner_send(k).wait_send()
        wait_for(tsend.at[k, pl.ds(0, IN_PLANE - 1)], tsent.at[k])
        wait_for(dsend.at[k, pl.ds(0, RING - 1)], dsent.at[k])
    wait_for(wrows.at[pl.ds(0, HALF - 1)], wsent)


def body(inverse_rows, factor, diag_inverse, pole_weights, structure, row_owner):
    rows = inverse_rows.reshape(2 * ROWS, inverse_rows.shape[3])
    by_pole = factor.reshape(SNODES, SHARD, 2, POLES, 64).transpose(0, 1, 3, 2, 4)
    by_pole = by_pole.reshape(SNODES, SHARD, 2 * BLOCK)
    diag = diag_inverse[0].transpose(0, 2, 3, 1)
    hbm = pl.BlockSpec(memory_space=pltpu.HBM)
    vmem = pl.BlockSpec(memory_space=pltpu.VMEM)
    dma = pltpu.SemaphoreType.DMA
    column, diagonal = pl.pallas_call(
        kernel,
        out_shape=(
            pltpu.VMEM((SNODES, 2, 64, ROWS), jnp.float32),
            pltpu.VMEM((SNODES, 2, 8, 64), jnp.float32),
        ),
        in_specs=[hbm, hbm, hbm, vmem, hbm, vmem],
        out_specs=(vmem, vmem),
        scratch_shapes=[
            pltpu.SMEM((SNODES, LISTED), jnp.int32),
            pltpu.SMEM((16,), jnp.int32),
            pltpu.SMEM((1, 2), jnp.float32),
            dma((3,)),
            pltpu.VMEM((SNODES, 64, SHARD, 2 * BLOCK), jnp.bfloat16),
            pltpu.VMEM((2 * ROWS, 8192), jnp.bfloat16),
            pltpu.VMEM((SNODES, POLES, ROWS, LANES), jnp.bfloat16),
            pltpu.VMEM((SNODES, POLES, ROWS, LANES), jnp.bfloat16),
            pltpu.VMEM((SNODES, ROWS, LANES), jnp.bfloat16),
            pltpu.VMEM((SNODES, ROWS, LANES), jnp.bfloat16),
            pltpu.VMEM((SNODES, IN_PLANE, SHARD, LANES), jnp.bfloat16),
            pltpu.VMEM((SNODES, IN_PLANE, SHARD, LANES), jnp.bfloat16),
            pltpu.VMEM((SNODES, RING, 8, LANES), jnp.bfloat16),
            pltpu.VMEM((SNODES, RING, 8, LANES), jnp.bfloat16),
            pltpu.VMEM((POLES, 8, LANES), jnp.float32),
            dma,
            dma((4, 20)),
            dma((SNODES,)),
            dma((SNODES,)),
            dma((SNODES,)),
            dma((SNODES,)),
            dma((SNODES,)),
            dma((SNODES,)),
            dma,
            dma((SNODES,)),
            dma((SNODES,)),
            dma((SNODES,)),
            dma((SNODES,)),
            dma((SNODES,)),
            dma((SNODES,)),
            dma,
        ],
        compiler_params=pltpu.CompilerParams(
            collective_id=0, has_side_effects=True, vmem_limit_bytes=60 * 1024 * 1024
        ),
    )(structure, row_owner, pole_weights, by_pole, rows, diag)
    column_sum = column.transpose(0, 3, 1, 2)
    diagonal_sum = diagonal.transpose(0, 3, 1, 2)
    return (column_sum, diagonal_sum)


def solution(mesh):
    in_specs = (
        P("pole", None, "grid", None),
        P("pole", None, "grid", None, None),
        P("pole", None, None, None, "grid"),
        P("pole", None),
        P(),
        P(),
    )
    out_specs = (P(None, "grid", None, "pole"), P(None, "pole", None, "grid"))
    return jax.shard_map(body, mesh=mesh, in_specs=in_specs, out_specs=out_specs, check_vma=False)
```

```python
import jax
import jax.numpy as jnp
from jax import lax
from jax.experimental import pallas as pl
from jax.experimental.pallas import tpu as pltpu
from jax.sharding import PartitionSpec as P

BLOCK = 512
LISTED = 4
SNODES = 2
POLES = 8
HALF = 4
PLANES = 2
SIDE = 4
IN_PLANE = 32
RING = 16
LANES = 128
ROWS = 128
SHARD = 32
MESH = pl.DeviceIdType.MESH
DOT = (((1,), (0,)), ((), ()))

ORDER = (
    (0, 0), (0, 2), (1, 0), (1, 2), (2, 0), (2, 2), (0, 1), (3, 0), (3, 2), (1, 1), (4, 0), (4, 2),
    (0, 3), (2, 1), (1, 3), (3, 1), (2, 3), (4, 1), (3, 3), "first", (4, 3), "second", "moments",
)
ROUNDS = ((0, 0), (0, 1), (1, 0), (1, 1))


def kernel(
    structure_hbm, row_owner_hbm, weights_hbm, factor, rows_hbm, diag,
    column_out, diag_out,
    structure, row_owner, weights, small_sem, fbuf, rows, esend, erecv, psend, precv, tsend, trecv, dsend, drecv, wrows,
    rows_sem, ag_sem, cross_sem, pair_sem, erecv_sem, precv_sem, trecv_sem, drecv_sem, wrecv_sem,
    ag_sent, cross_sent, esent, psent, tsent, dsent, wsent,
):
    pole = lax.axis_index("pole")
    grid = lax.axis_index("grid")
    x, plane = grid // 16, (grid // 8) % 2
    y, core = (grid // 2) % 4, grid % 2
    seat = x * 8 + y * 2 + core
    height = plane * 8 + pole
    quad, member = pole // HALF, pole % HALF

    def at(x_to, plane_to, y_to, core_to):
        return x_to * 16 + plane_to * 8 + y_to * 2 + core_to

    def along(first, second, core_to=core, plane_to=plane):
        x_to = (x + core * first + (1 - core) * second) % SIDE
        y_to = (y + (1 - core) * first + core * second) % SIDE
        return at(x_to, plane_to, y_to, core_to)

    def seat_grid(seat_to):
        return at(seat_to // 8, plane, (seat_to // 2) % 4, seat_to % 2)

    def height_device(height_to):
        return (height_to % 8, at(x, height_to // 8, y, core))

    load_rows = pltpu.make_async_copy(rows_hbm, rows, rows_sem)
    load_rows.start()
    small = [
        pltpu.make_async_copy(source, target, small_sem.at[i])
        for i, (source, target) in enumerate(
            ((structure_hbm, structure), (row_owner_hbm, row_owner), (weights_hbm, weights))
        )
    ]
    for load in small:
        load.start()

    barrier = pltpu.get_barrier_semaphore()

    beside = [along(1, 0), along(-1, 0), along(0, 1), along(0, -1), at(x, plane, y, 1 - core)]

    def greet_height(step, carry):
        target = height_device((height + step) % RING)
        pl.semaphore_signal(barrier, inc=1, device_id=target, device_id_type=MESH)
        return carry

    lax.fori_loop(8, RING, greet_height, 0)
    lax.fori_loop(1, 8, greet_height, 0)
    for target in beside:
        pl.semaphore_signal(barrier, inc=1, device_id=(pole, target), device_id_type=MESH)
    for k in range(SNODES):
        fbuf[k, grid] = factor[k]
    for load in small:
        load.wait()
    part = lax.broadcasted_iota(jnp.int32, (8, LANES), 0)
    wrows[pole] = jnp.where(part == 0, weights[0, 0], weights[0, 1])
    pl.semaphore_wait(barrier, len(beside) + RING - 1)

    def copy(src, dst, sent, received, device):
        return pltpu.make_async_remote_copy(
            src_ref=src, dst_ref=dst, send_sem=sent, recv_sem=received,
            device_id=device, device_id_type=MESH,
        )

    def cross(k):
        return copy(
            factor.at[k], fbuf.at[k, grid], cross_sent.at[k], cross_sem.at[k],
            height_device((height + 8) % RING),
        )

    for k in range(SNODES):
        cross(k).start()

    def wait_for(ref, sem):
        pltpu.make_async_copy(ref, ref, sem).wait()

    def push(r, src, slot, offset, sem_index):
        k = ROUNDS[r][0]
        first, second = offset
        copy(
            src, slot, ag_sent.at[k], ag_sem.at[r, sem_index],
            (pole, along(first, second)),
        ).start()

    def stage(step, r):
        k, other = ROUNDS[r]
        source_plane = plane if other == 0 else 1 - plane

        def shard(first, second):
            return fbuf.at[k, along(first, second, plane_to=source_plane)]

        def half(ref, which):
            return ref.at[pl.ds(16 * which, 16)]

        own = factor.at[k] if other == 0 else shard(0, 0)

        def to_sibling(src, first, second):
            copy(
                src, shard(first, second), ag_sent.at[k], pair_sem.at[k],
                (pole, at(x, plane, y, 1 - core)),
            ).start()

        def start_second(src, first, index):
            slot = shard(first, 0)
            push(r, src, slot, (0, 1), 4 + 4 * index)
            push(r, src, slot, (0, -1), 5 + 4 * index)

        def turn_second(first, index):
            base = 4 + 4 * index
            low = shard(first, -1)
            wait_for(low, ag_sem.at[r, base])
            push(r, half(low, 0), half(low, 0), (0, 1), base + 2)
            to_sibling(low, first, -1)
            high = shard(first, 1)
            wait_for(high, ag_sem.at[r, base + 1])
            push(r, half(high, 1), half(high, 1), (0, -1), base + 3)
            to_sibling(high, first, 1)

        def end_second(first, index):
            base = 4 + 4 * index
            far = shard(first, 2)
            wait_for(half(far, 0), ag_sem.at[r, base + 2])
            wait_for(half(far, 1), ag_sem.at[r, base + 3])
            to_sibling(far, first, 2)

        if step == 0:
            if other == 1:
                cross(k).wait_recv()
            push(r, own, shard(0, 0), (1, 0), 0)
            push(r, own, shard(0, 0), (-1, 0), 1)
            start_second(own, 0, 0)
            to_sibling(own, 0, 0)
        if step == 1:
            low = shard(-1, 0)
            wait_for(low, ag_sem.at[r, 0])
            push(r, half(low, 0), half(low, 0), (1, 0), 2)
            start_second(low, -1, 1)
            to_sibling(low, -1, 0)
            high = shard(1, 0)
            wait_for(high, ag_sem.at[r, 1])
            push(r, half(high, 1), half(high, 1), (-1, 0), 3)
            start_second(high, 1, 2)
            to_sibling(high, 1, 0)
            turn_second(0, 0)
        if step == 2:
            far = shard(2, 0)
            wait_for(half(far, 0), ag_sem.at[r, 2])
            wait_for(half(far, 1), ag_sem.at[r, 3])
            start_second(far, 2, 3)
            to_sibling(far, 2, 0)
            turn_second(-1, 1)
            turn_second(1, 2)
            end_second(0, 0)
        if step == 3:
            turn_second(2, 3)
            end_second(-1, 1)
            end_second(1, 2)
        if step == 4:
            end_second(2, 3)

    lane = lax.broadcasted_iota(jnp.int32, (1, LANES), 1)
    sign = jnp.where(lane < 64, -1.0, 1.0).astype(jnp.float32)

    def turned(values):
        return sign * pltpu.roll(values, 64, 1)

    def weight_send(step):
        return copy(
            wrows.at[pole], wrows.at[pole], wsent, wrecv_sem,
            (quad * HALF + (member + step) % HALF, grid),
        )

    def columns(k):
        wait_for(fbuf.at[k, pl.ds(0, IN_PLANE)], pair_sem.at[k])
        active = 0
        for i in range(LISTED):
            active = active + jnp.where(owners[k][i] == grid // 4, 1, 0)
        active = active.astype(jnp.float32)

        def chunk(step, carry):
            n = (x + 1 + step) % SIDE
            start = pl.multiple_of(2 * LANES * n, 2 * LANES)
            product = jnp.zeros((2 * ROWS, 2 * LANES), jnp.float32)
            for i in range(LISTED):
                block = fbuf[k, pl.ds(16 * i, 16), :, pl.ds(start, 2 * LANES)]
                product = product + lax.dot_general(
                    rows[:, pl.ds(structure[k, i] * BLOCK, BLOCK)],
                    block.reshape(BLOCK, 2 * LANES),
                    DOT,
                    preferred_element_type=jnp.float32,
                )
            flipped = []
            for u in range(2):
                lanes = slice(LANES * u, LANES * (u + 1))
                value = -(product[:ROWS, lanes] + turned(product[ROWS:, lanes]))
                rounded = (value * active).astype(jnp.bfloat16)
                esend[k, 2 * n + u] = rounded
                flipped.append(jnp.transpose(rounded.astype(jnp.float32)))
            for h in range(8):
                pieces = [
                    flipped[u][64 * part_id + 8 * h : 64 * part_id + 8 * h + 8]
                    for part_id in range(2)
                    for u in range(2)
                ]
                tsend[k, 8 * n + h] = jnp.concatenate(pieces, axis=0).astype(jnp.bfloat16)

            def send_tile(h, inner):
                target = 8 * n + (y * 2 + core + 1 + h) % 8

                @pl.when(target != seat)
                def _():
                    copy(
                        tsend.at[k, target], trecv.at[k, seat], tsent.at[k], trecv_sem.at[k],
                        (pole, seat_grid(target)),
                    ).start()

                return inner

            lax.fori_loop(0, 8, send_tile, 0)
            for u in range(2):
                chunk_id = 2 * n + u
                owner = chunk_id % HALF
                slot = (chunk_id // HALF) * HALF + member

                @pl.when(owner != member)
                def _(chunk_id=chunk_id, owner=owner, slot=slot):
                    copy(
                        esend.at[k, chunk_id], erecv.at[k, slot], esent.at[k], erecv_sem.at[k],
                        (quad * HALF + owner, grid),
                    ).start()

            return carry

        lax.fori_loop(0, SIDE, chunk, 0)
        for part in range(2):
            erecv[k, part * HALF + member] = esend[k, part * HALF + member]
        trecv[k, seat] = tsend[k, seat]

    def moments(k):
        wait_for(trecv.at[k, pl.ds(0, IN_PLANE - 1)], trecv_sem.at[k])
        total = jnp.zeros((SHARD, 2 * BLOCK), jnp.float32)
        for i in range(LISTED):
            left = jnp.zeros((SHARD, BLOCK), jnp.bfloat16)
            for slot in range(8):
                place = (slot // 2) * 4 + plane * 2 + slot % 2
                here = jnp.where(owners[k][i] == place, 1.0, 0.0).astype(jnp.bfloat16)
                tiles = [trecv[k, 4 * slot + q] for q in range(4)]
                left = left + here * jnp.concatenate(tiles, axis=1)
            block = fbuf[k, pl.ds(16 * i, 16)].reshape(BLOCK, 2 * BLOCK)
            total = total + lax.dot_general(left, block, DOT, preferred_element_type=jnp.float32)
        weight_real, weight_imag = weights[0, 0], weights[0, 1]
        for j in range(POLES):
            lanes = slice(LANES * j, LANES * (j + 1))
            moment = total[:16, lanes] + turned(total[16:, lanes])
            at_128 = slice(LANES * (j // 2), LANES * (j // 2 + 1))
            diag_real, diag_imag = diag[k, 0, :, at_128], diag[k, 1, :, at_128]
            if j % 2 == 0:
                given = jnp.where(lane < 64, diag_real, pltpu.roll(diag_imag, 64, 1))
            else:
                given = jnp.where(lane < 64, pltpu.roll(diag_real, 64, 1), diag_imag)
            for side in range(2):
                mine = jnp.where(plane == side, 1.0, 0.0).astype(jnp.float32)
                value = mine * given - moment[8 * side : 8 * side + 8]
                weighted = weight_real * value + weight_imag * turned(value)
                dsend[k, 8 * side + j] = weighted.astype(jnp.bfloat16)

        def send_diag(step, carry):
            target = (height + step) % RING
            copy(
                dsend.at[k, target], drecv.at[k, height], dsent.at[k], drecv_sem.at[k],
                height_device(target),
            ).start()
            return carry

        lax.fori_loop(1, RING, send_diag, 0)
        drecv[k, height] = dsend[k, height]

    def partner_send(k):
        return copy(
            psend.at[k], precv.at[k], psent.at[k], precv_sem.at[k],
            ((pole + HALF) % POLES, grid),
        )

    def half_sum(k, part):
        straight = jnp.zeros((ROWS, LANES), jnp.float32)
        crossed = jnp.zeros((ROWS, LANES), jnp.float32)
        for r in range(HALF):
            value = erecv[k, part * HALF + r].astype(jnp.float32)
            straight = straight + wrows[quad * HALF + r, 0:1, :] * value
            crossed = crossed + wrows[quad * HALF + r, 1:2, :] * value
        return straight + turned(crossed)

    def send_half(k):
        wait_for(erecv.at[k, pl.ds(0, 2 * HALF - 2)], erecv_sem.at[k])
        psend[k] = half_sum(k, 1 - quad).astype(jnp.bfloat16)
        partner_send(k).start()

    def sum_columns(k):
        own = half_sum(k, quad)
        partner_send(k).wait_recv()
        flat = jnp.transpose(own + precv[k].astype(jnp.float32))
        column_out[k, 0] = flat[:64]
        column_out[k, 1] = flat[64:]

    owners = []
    for k in range(SNODES):
        owners.append([])
        for i in range(LISTED):
            owner = 0
            for ancestor in range(16):
                owner = owner + jnp.where(structure[k, i] == ancestor, row_owner[ancestor], 0)
            owners[k].append(owner)

    for step in range(1, HALF):
        weight_send(step).start()

    for entry in ORDER:
        if entry == "first":
            load_rows.wait()
            columns(0)
        elif entry == "second":
            columns(1)
        elif entry == "moments":
            moments(0)
        else:
            stage(*entry)

    wait_for(wrows.at[pl.ds(0, HALF - 1)], wrecv_sem)
    send_half(0)
    moments(1)
    send_half(1)
    sum_columns(0)
    sum_columns(1)
    for k in range(SNODES):
        wait_for(drecv.at[k, pl.ds(0, RING - 1)], drecv_sem.at[k])
        summed = drecv[k, 0].astype(jnp.float32)
        for source in range(1, RING):
            summed = summed + drecv[k, source].astype(jnp.float32)
        diag_out[k, 0] = summed[:, :64]
        diag_out[k, 1] = pltpu.roll(summed, 64, 1)[:, :64]

    for k in range(SNODES):
        cross(k).wait_send()
        wait_for(fbuf.at[k, pl.ds(0, 62)], ag_sent.at[k])
        wait_for(esend.at[k, pl.ds(0, 2 * HALF - 2)], esent.at[k])
        partner_send(k).wait_send()
        wait_for(tsend.at[k, pl.ds(0, IN_PLANE - 1)], tsent.at[k])
        wait_for(dsend.at[k, pl.ds(0, RING - 1)], dsent.at[k])
    wait_for(wrows.at[pl.ds(0, HALF - 1)], wsent)


def body(inverse_rows, factor, diag_inverse, pole_weights, structure, row_owner):
    rows = inverse_rows.reshape(2 * ROWS, inverse_rows.shape[3])
    by_pole = factor.reshape(SNODES, SHARD, 2, POLES, 64).transpose(0, 1, 3, 2, 4)
    by_pole = by_pole.reshape(SNODES, SHARD, 2 * BLOCK)
    diag = diag_inverse[0].transpose(0, 2, 3, 1)
    hbm = pl.BlockSpec(memory_space=pltpu.HBM)
    vmem = pl.BlockSpec(memory_space=pltpu.VMEM)
    dma = pltpu.SemaphoreType.DMA
    column, diagonal = pl.pallas_call(
        kernel,
        out_shape=(
            pltpu.VMEM((SNODES, 2, 64, ROWS), jnp.float32),
            pltpu.VMEM((SNODES, 2, 8, 64), jnp.float32),
        ),
        in_specs=[hbm, hbm, hbm, vmem, hbm, vmem],
        out_specs=(vmem, vmem),
        scratch_shapes=[
            pltpu.SMEM((SNODES, LISTED), jnp.int32),
            pltpu.SMEM((16,), jnp.int32),
            pltpu.SMEM((1, 2), jnp.float32),
            dma((3,)),
            pltpu.VMEM((SNODES, 64, SHARD, 2 * BLOCK), jnp.bfloat16),
            pltpu.VMEM((2 * ROWS, 8192), jnp.bfloat16),
            pltpu.VMEM((SNODES, POLES, ROWS, LANES), jnp.bfloat16),
            pltpu.VMEM((SNODES, POLES, ROWS, LANES), jnp.bfloat16),
            pltpu.VMEM((SNODES, ROWS, LANES), jnp.bfloat16),
            pltpu.VMEM((SNODES, ROWS, LANES), jnp.bfloat16),
            pltpu.VMEM((SNODES, IN_PLANE, SHARD, LANES), jnp.bfloat16),
            pltpu.VMEM((SNODES, IN_PLANE, SHARD, LANES), jnp.bfloat16),
            pltpu.VMEM((SNODES, RING, 8, LANES), jnp.bfloat16),
            pltpu.VMEM((SNODES, RING, 8, LANES), jnp.bfloat16),
            pltpu.VMEM((POLES, 8, LANES), jnp.float32),
            dma,
            dma((4, 20)),
            dma((SNODES,)),
            dma((SNODES,)),
            dma((SNODES,)),
            dma((SNODES,)),
            dma((SNODES,)),
            dma((SNODES,)),
            dma,
            dma((SNODES,)),
            dma((SNODES,)),
            dma((SNODES,)),
            dma((SNODES,)),
            dma((SNODES,)),
            dma((SNODES,)),
            dma,
        ],
        compiler_params=pltpu.CompilerParams(
            collective_id=0, has_side_effects=True, vmem_limit_bytes=60 * 1024 * 1024
        ),
    )(structure, row_owner, pole_weights, by_pole, rows, diag)
    column_sum = column.transpose(0, 3, 1, 2)
    diagonal_sum = diagonal.transpose(0, 3, 1, 2)
    return (column_sum, diagonal_sum)


def solution(mesh):
    in_specs = (
        P("pole", None, "grid", None),
        P("pole", None, "grid", None, None),
        P("pole", None, None, None, "grid"),
        P("pole", None),
        P(),
        P(),
    )
    out_specs = (P(None, "grid", None, "pole"), P(None, "pole", None, "grid"))
    return jax.shard_map(body, mesh=mesh, in_specs=in_specs, out_specs=out_specs, check_vma=False)
```
